256 devices in a mesh: dp: 8 (over z), head: 32 (over y, x, core).
Axes of the slice: x: 4, y: 4, z: 8, core: 2. Of those that a mesh axis runs over, the one named last changes fastest.
Arguments:
- residual: float32 [192, 4096], P('dp', 'head'), parts along dimension 0, may hold values from -70 to 70
- norm_gain: float32 [4096], replicated, may hold values from 0.5 to 1.5
- w_query: bfloat16 [8, 256, 4096], P(None, 'head'), may hold values from -0.09375 to 0.09375
- w_key: bfloat16 [8, 256, 4096], P(None, 'head'), may hold values from -0.09375 to 0.09375
- w_value: bfloat16 [4096, 4096], P(None, 'head'), may hold values from -0.09375 to 0.09375
- w_gate: bfloat16 [4096, 4096], P(None, 'head'), may hold values from -0.09375 to 0.09375
- w_input: bfloat16 [8, 4096], replicated, may hold values from -0.09375 to 0.09375
- w_forget: bfloat16 [8, 4096], replicated, may hold values from -0.09375 to 0.09375
- b_input: float32 [8], replicated, may hold values from -2 to -0.5
- b_forget: float32 [8], replicated, may hold values from 0.5 to 4
- w_out: bfloat16 [4096, 4096], P('head'), may hold values from -0.1875 to 0.1875
- memory: bfloat16 [192, 8, 256, 512], P('dp', None, 'head'), parts along dimension 0, may hold values from -0.59765625 to 0.59765625
- normalizer: float32 [192, 8, 256], P('dp', None, 'head'), parts along dimension 0, may hold values from -0.6 to 0.6
- stabilizer: float32 [192, 8], P('dp'), parts along dimension 0, may hold values from -0.5 to 0.5
Outputs:
- res_out: float32 [192, 4096], P('dp', 'head'), parts along dimension 0
- mem_out: bfloat16 [192, 8, 256, 512], P('dp', None, 'head'), parts along dimension 0
- norm_out: float32 [192, 8, 256], P('dp', None, 'head'), parts along dimension 0
- stab_out: float32 [192, 8], P('dp'), parts along dimension 0
The draws below stay inside these ranges and needn't reach their ends.
There are 8 independent parts, one for each index of `dp`. The reference program is written for one: setup_inputs(seed, part) draws one part's arguments, and reference() takes and returns one part's arrays. A program takes and returns all parts, laid end to end along the dimension named above; an argument that names none is the same for every part. Nothing has to cross between parts.
All inputs are finite; a program needn't handle non-finite values.
Results may differ from the reference program's by a relative error of at most 0.0095.
Values may be sent and summed in bfloat16 or wider, within the bound.
No kernel may reach another device: no remote copies, remote signals or barrier semaphores. Data moves between devices by JAX's collectives and lax.ppermute only.
A program may use at most 64 MiB of HBM per device.

```python
import math
import jax
import jax.numpy as jnp
from jax import lax

D = 4096
H = 8
DK = 256
DV = 512
B = 24


def draw_residual(key, part):
    key_base = jax.random.fold_in(key, 11)
    key_cols = jax.random.fold_in(key, 12)
    key_rows = jax.random.fold_in(key, 13)
    position = jnp.arange(D, dtype=jnp.float32) / D
    col_log = 0.5 * jnp.log(3.0) * position + jax.random.uniform(key_cols, (D,), jnp.float32, -1.15, 1.15)
    row_log = jax.random.uniform(key_rows, (B,), jnp.float32, -0.6, 0.6)
    base_vals = jax.random.truncated_normal(key_base, -4.0, 4.0, (B, D), jnp.float32)
    return base_vals * jnp.exp(row_log[:, None] + col_log[None, :])


def strengthened(result, own_key, source, target, shards_of, factor):
    owner, partner = [(jnp.arange(result.shape[dim]) // (result.shape[dim] // shards_of)).reshape([-1 if axis == dim else 1 for axis in range(result.ndim)]) for dim in (source, target)]
    chosen = jax.random.permutation(own_key, shards_of)[partner]
    strong = (owner == chosen) | (owner == (partner + shards_of // 2) % shards_of)
    return jnp.where(strong, factor * result, result)


def steps_of(rng, dims, pieces, low, high):
    level = 1.0
    for axis_at, parts in pieces:
        heights = jax.random.uniform(jax.random.fold_in(jax.random.fold_in(rng, 6), axis_at), (parts,), jnp.float32, low / len(pieces), high / len(pieces))
        level = level * jnp.repeat(jnp.exp(heights), dims[axis_at] // parts).reshape((-1,) + (1,) * (len(dims) - 1 - axis_at))
    return level


def bell_draw(rng, extent, deviation, bound, shards=(), kind=jnp.bfloat16):
    drawn = deviation * jax.random.normal(rng, extent, jnp.float32)
    if shards:
        drawn = drawn * steps_of(rng, extent, shards, -0.22, 0.18)
    return jnp.clip(drawn, -bound, bound).astype(kind)


def heavy_noise(key, extent, width, most, shards, heavy, kind=jnp.bfloat16):
    values = width * jax.random.normal(key, extent, jnp.float32)
    if shards:
        values = values * steps_of(key, extent, shards, -0.22, 0.18)
    return jnp.clip(strengthened(values, jax.random.fold_in(key, 3), *heavy), -most, most).astype(kind)


def setup_inputs(seed: int = 0, part: int = 0) -> dict:
    keys = jax.random.split(jax.random.key(seed), 15)
    part_keys = jax.random.split(jax.random.fold_in(keys[14], part), 15)
    residual = draw_residual(jax.random.fold_in(jax.random.fold_in(keys[14], part), 71), part)
    norm_gain = jnp.clip(1.0 + 0.1 * jax.random.normal(keys[1], (D,), jnp.float32), 0.5, 1.5)
    w_query = bell_draw(keys[2], (H, DK, D), D ** -0.5, 0.09375, ((1, 32),))
    w_key = bell_draw(keys[3], (H, DK, D), D ** -0.5, 0.09375, ((1, 32),))
    w_value = bell_draw(keys[4], (D, H * DV), D ** -0.5, 0.09375, ((1, 32),))
    w_gate = bell_draw(keys[5], (D, H * DV), D ** -0.5, 0.09375, ((1, 32),))
    w_input = bell_draw(keys[6], (H, D), D ** -0.5, 0.09375)
    w_forget = bell_draw(keys[7], (H, D), D ** -0.5, 0.09375)
    b_input = jnp.clip(jax.random.uniform(keys[8], (H,), jnp.float32, -2.0, -0.5), -2.0, -0.5)
    b_forget = jnp.clip(jax.random.uniform(keys[9], (H,), jnp.float32, 0.5, 4.0), 0.5, 4.0)
    w_out = heavy_noise(keys[10], (H * DV, D), (H * DV) ** -0.5, 0.1875, ((0, 32),), (0, 1, 32, 2.75))
    memory = heavy_noise(part_keys[11], (B, H, DK, DV), 0.1, 0.59765625, ((2, 32),), (2, 3, 32, 2.75))
    normalizer = bell_draw(part_keys[12], (B, H, DK), 0.1, 0.6, ((2, 32),), jnp.float32)
    stabilizer = jnp.clip(jax.random.uniform(part_keys[13], (B, H), jnp.float32, -0.5, 0.5), -0.5, 0.5)
    return dict(residual=residual, norm_gain=norm_gain, w_query=w_query, w_key=w_key, w_value=w_value, w_gate=w_gate, w_input=w_input, w_forget=w_forget, b_input=b_input, b_forget=b_forget, w_out=w_out, memory=memory, normalizer=normalizer, stabilizer=stabilizer)


epsilon = 1e-06

def reference(residual, norm_gain, w_query, w_key, w_value, w_gate, w_input, w_forget, b_input, b_forget, w_out, memory, normalizer, stabilizer):
    mean_sq = lax.optimization_barrier(jnp.mean(residual * residual, axis=1, keepdims=True))
    x_norm = (residual * lax.rsqrt(mean_sq + epsilon) * norm_gain).astype(jnp.bfloat16)
    x_wide = x_norm.astype(jnp.float32)
    query_vec = jnp.einsum('bd,hkd->bhk', x_wide, w_query.astype(jnp.float32))
    key_vec = jnp.einsum('bd,hkd->bhk', x_wide, w_key.astype(jnp.float32)) / math.sqrt(DK)
    value_vec = jnp.dot(x_norm, w_value, preferred_element_type=jnp.float32).astype(jnp.bfloat16)
    input_pre = jnp.dot(x_norm, w_input.T, preferred_element_type=jnp.float32) + b_input
    forget_pre = jnp.dot(x_norm, w_forget.T, preferred_element_type=jnp.float32) + b_forget
    log_forget = jax.nn.log_sigmoid(forget_pre)
    stab_new = jnp.maximum(log_forget + stabilizer, input_pre)
    input_gate = jnp.exp(input_pre - stab_new)
    forget_gate = jnp.exp(log_forget + stabilizer - stab_new)
    batch_size = residual.shape[0]
    value_heads = value_vec.astype(jnp.float32).reshape(batch_size, H, DV)
    memory_full = forget_gate[:, :, None, None] * memory.astype(jnp.float32) + input_gate[:, :, None, None] * key_vec[:, :, :, None] * value_heads[:, :, None, :]
    norm_new = forget_gate[:, :, None] * normalizer + input_gate[:, :, None] * key_vec
    numerator = lax.optimization_barrier(jnp.sum(memory_full * query_vec[:, :, :, None], axis=2))
    denom_all = lax.optimization_barrier(jnp.sum(norm_new * query_vec, axis=2))
    readout = numerator / jnp.maximum(jnp.abs(denom_all), jnp.exp(-stab_new))[:, :, None]
    out_gate = jax.nn.sigmoid(jnp.dot(x_norm, w_gate, preferred_element_type=jnp.float32))
    hidden = (out_gate * readout.reshape(batch_size, H * DV)).astype(jnp.bfloat16)
    res_out = residual + jnp.dot(hidden, w_out, preferred_element_type=jnp.float32)
    return (res_out, memory_full.astype(jnp.bfloat16), norm_new, stab_new)
```

```python
import math

import jax
import jax.numpy as jnp
from jax import lax
from jax.experimental import pallas as pl
from jax.experimental.pallas import tpu as pltpu
from jax.sharding import PartitionSpec as P

H = 8
DK = 256
DV = 512
EPSILON = 1e-06
F32 = jnp.float32
BF16 = jnp.bfloat16
STATS = 8


def exchange(pieces):
    return lax.all_to_all(pieces, "head", 0, 0, tiled=True)


def dot_last(left, right):
    return lax.dot_general(left, right, (((1,), (1,)), ((), ())), preferred_element_type=F32)


def dot(left, right):
    return jnp.dot(left, right, preferred_element_type=F32)


def column(row):
    n = row.shape[1]
    at_row = lax.broadcasted_iota(jnp.int32, (n, n), 0)
    at_col = lax.broadcasted_iota(jnp.int32, (n, n), 1)
    return jnp.sum(jnp.where(at_row == at_col, row, 0.0), axis=1, keepdims=True)


def split_hi_lo(value):
    high = value.astype(BF16).astype(F32)
    return high, value - high


def project_kernel(
    x_ref, gain_ref, wq_ref, wk_ref, wv_ref, wi_ref, wf_ref, bi_ref, bf_ref, mem_ref, nrm_ref, stab_ref,
    out_ref, value_ref, xn_ref, nrm_out_ref, stab_out_ref, fg_ref, ig_ref, f_rows_ref, ik_rows_ref,
    stats_ref,
):
    pieces, batch, width = x_ref.shape
    rows = wq_ref.shape[0] // H
    total = jnp.zeros((batch, width), F32)
    for j in range(pieces):
        x = x_ref[j].astype(F32)
        total = total + x * x
    mean = jnp.sum(total, axis=1, keepdims=True) / (pieces * width)
    scale = lax.rsqrt(mean + EPSILON)
    for j in range(pieces):
        cut = slice(j * width, (j + 1) * width)
        xn_ref[:, cut] = (x_ref[j].astype(F32) * scale * gain_ref[:, cut]).astype(BF16)
    x_norm = xn_ref[...]

    query = dot_last(x_norm, wq_ref[...])
    query_t = dot_last(wq_ref[...], x_norm)
    key_t = dot_last(wk_ref[...], x_norm) / math.sqrt(DK)
    input_pre = dot_last(wi_ref[...], x_norm) + column(bi_ref[...])
    forget_pre = dot_last(wf_ref[...], x_norm) + column(bf_ref[...])
    value = dot(x_norm, wv_ref[...]).astype(BF16)
    for j in range(pieces):
        value_ref[j] = value

    log_forget = jnp.minimum(forget_pre, 0.0) - jnp.log1p(jnp.exp(-jnp.abs(forget_pre)))
    kept = log_forget + stab_ref[...]
    stab_new = jnp.maximum(kept, input_pre)
    input_gate = jnp.exp(input_pre - stab_new)
    forget_gate = jnp.exp(kept - stab_new)
    stab_out_ref[...] = stab_new
    fg_ref[...] = forget_gate
    ig_ref[...] = input_gate

    stats_ref[...] = jnp.zeros(stats_ref.shape, F32)
    for h in range(H):
        part = slice(h * rows, (h + 1) * rows)
        key_h = key_t[part]
        query_h = query_t[part]
        f_h = jnp.broadcast_to(forget_gate[h : h + 1], (rows, batch))
        ik_h = input_gate[h : h + 1] * key_h
        norm_h = f_h * nrm_ref[part] + ik_h
        nrm_out_ref[part] = norm_h
        f_rows_ref[part] = f_h
        ik_rows_ref[part] = ik_h
        norm_query = jnp.sum(norm_h * query_h, axis=0, keepdims=True)
        key_query = jnp.sum(key_h * query_h, axis=0, keepdims=True)
        kinds = (*split_hi_lo(norm_query), *split_hi_lo(key_query))
        for k, kind in enumerate(kinds):
            stats_ref[h, k : k + 1, :batch] = kind

    spread = batch * rows
    high, low = split_hi_lo(query)
    both = jnp.concatenate([high, low], axis=0).astype(BF16)
    at_k = lax.broadcasted_iota(jnp.int32, (rows, spread), 0)
    at_n = lax.broadcasted_iota(jnp.int32, (rows, spread), 1)
    repeat = jnp.where(at_n % rows == at_k, 1.0, 0.0).astype(BF16)
    own_b = lax.broadcasted_iota(jnp.int32, (2 * batch, spread), 0) % batch
    own_n = lax.broadcasted_iota(jnp.int32, (2 * batch, spread), 1) // rows
    own = own_b == own_n
    share = pieces // H
    for h in range(H):
        wide = dot(both[:, h * rows : (h + 1) * rows], repeat)
        left = jnp.where(own, wide, 0.0).astype(BF16)
        memory = mem_ref[:, h].astype(F32).reshape(spread, share * width).astype(BF16)
        product = dot(left, memory)
        numer = (product[:batch] + product[batch:]).astype(BF16)
        stats = stats_ref[h].astype(BF16)
        for c in range(share):
            out_ref[h * share + c, :batch] = numer[:, c * width : (c + 1) * width]
            out_ref[h * share + c, batch:] = stats


def gate_kernel(head_ref, xn_ref, wg_ref, value_ref, fg_ref, ig_ref, stab_ref, sum_scale_ref, own_ref, floor_ref):
    head = head_ref[0]
    pick = lambda ref: column(ref[pl.ds(head, 1), :])
    gate = jax.nn.sigmoid(dot(xn_ref[...], wg_ref[...]))
    sum_scale_ref[...] = gate * pick(fg_ref)
    own_ref[...] = gate * pick(ig_ref) * value_ref[0].astype(F32)
    floor_ref[...] = jnp.broadcast_to(jnp.exp(-pick(stab_ref)), floor_ref.shape)


def output_kernel(in_ref, sum_scale_ref, own_ref, floor_ref, wo_ref, out_ref):
    pieces, batch, width = out_ref.shape
    total = jnp.zeros(in_ref.shape[1:], F32)
    for j in range(pieces):
        total = total + in_ref[j].astype(F32)
    norm_query = column(total[batch : batch + 1, :batch] + total[batch + 1 : batch + 2, :batch])
    key_query = column(total[batch + 2 : batch + 3, :batch] + total[batch + 3 : batch + 4, :batch])
    numer = sum_scale_ref[...] * total[:batch] + own_ref[...] * key_query
    hidden = (numer / jnp.maximum(jnp.abs(norm_query), floor_ref[...])).astype(BF16)
    for j in range(pieces):
        out_ref[j] = dot(hidden, wo_ref[:, j * width : (j + 1) * width]).astype(BF16)


def memory_kernel(mem_ref, value_ref, f_rows_ref, ik_rows_ref, out_ref, wide_ref):
    pieces, batch, width = value_ref.shape
    share = pieces // H
    rows = mem_ref.shape[2]
    for j in range(pieces):
        cut = slice((j % share) * width, (j % share + 1) * width)
        wide_ref[j // share, :, cut] = value_ref[j].astype(F32)

    def one_head(h, carry):
        at = pl.multiple_of(h * rows, rows)
        f_rows = f_rows_ref[pl.ds(at, rows), :]
        ik_rows = ik_rows_ref[pl.ds(at, rows), :]
        for b in range(batch):
            kept = f_rows[:, b : b + 1] * mem_ref[b, h].astype(F32)
            out_ref[b, h] = (kept + ik_rows[:, b : b + 1] * wide_ref[h, b : b + 1, :]).astype(BF16)
        return carry

    lax.fori_loop(0, H, one_head, 0)


def finish_kernel(in_ref, residual_ref, out_ref):
    total = residual_ref[...]
    acc = in_ref[0].astype(F32)
    for j in range(1, in_ref.shape[0]):
        acc = acc + in_ref[j].astype(F32)
    out_ref[...] = total + acc


def call(kernel, outs, n_in, scratch=(), smem=0, flops=1_000_000):
    return pl.pallas_call(
        kernel,
        out_shape=[jax.ShapeDtypeStruct(*out) for out in outs],
        in_specs=[pl.BlockSpec(memory_space=pltpu.SMEM)] * smem
        + [pl.BlockSpec(memory_space=pltpu.VMEM)] * n_in,
        out_specs=[pl.BlockSpec(memory_space=pltpu.VMEM)] * len(outs),
        scratch_shapes=list(scratch),
        compiler_params=pltpu.CompilerParams(vmem_limit_bytes=16 * 2**20),
        cost_estimate=pl.CostEstimate(flops=flops, bytes_accessed=2_000_000, transcendentals=0),
    )


def body(
    residual,
    norm_gain,
    w_query,
    w_key,
    w_value,
    w_gate,
    w_input,
    w_forget,
    b_input,
    b_forget,
    w_out,
    memory,
    normalizer,
    stabilizer,
):
    count = lax.axis_size("head")
    batch, width = residual.shape
    rows = w_query.shape[1]
    features = count * width
    head_mine = lax.axis_index("head") * width // DV
    gathered = exchange(jnp.broadcast_to(residual.astype(BF16)[None], (count, batch, width)))

    norm_t = normalizer.transpose(1, 2, 0).reshape(H * rows, batch)
    piece = ((count, batch, width), BF16)
    payload, values, x_norm, norm_new, stab_new, forget_gate, input_gate, f_rows, ik_rows = call(
        project_kernel,
        [
            ((count, batch + STATS, width), BF16),
            piece,
            ((batch, features), BF16),
            ((H * rows, batch), F32),
            ((H, batch), F32),
            ((H, batch), F32),
            ((H, batch), F32),
            ((H * rows, batch), F32),
            ((H * rows, batch), F32),
        ],
        12,
        scratch=[pltpu.VMEM((H, STATS, width), F32)],
        flops=100_000_000,
    )(
        gathered,
        norm_gain[None],
        w_query.reshape(H * rows, features),
        w_key.reshape(H * rows, features),
        w_value,
        w_input,
        w_forget,
        b_input[None],
        b_forget[None],
        memory,
        norm_t,
        stabilizer.T,
    )
    arrived = exchange(payload)
    value_heads = exchange(values)
    sum_scale, own, floor = call(
        gate_kernel, [((batch, width), F32)] * 3, 6, smem=1, flops=30_000_000
    )(head_mine[None].astype(jnp.int32), x_norm, w_gate, values, forget_gate, input_gate, stab_new)
    (branch,) = call(output_kernel, [piece], 5, flops=30_000_000)(
        arrived, sum_scale, own, floor, w_out
    )
    returned = exchange(branch)
    (mem_new,) = call(
        memory_kernel,
        [(memory.shape, BF16)],
        4,
        scratch=[pltpu.VMEM((H, batch, DV), F32)],
        flops=100_000_000,
    )(memory, value_heads, f_rows, ik_rows)
    (res_out,) = call(finish_kernel, [((batch, width), F32)], 2)(returned, residual)
    norm_out = norm_new.reshape(H, rows, batch).transpose(2, 0, 1)
    return res_out, mem_new, norm_out, stab_new.T


def solution(mesh):
    in_specs = (
        P("dp", "head"),
        P(),
        P(None, "head", None),
        P(None, "head", None),
        P(None, "head"),
        P(None, "head"),
        P(),
        P(),
        P(),
        P(),
        P("head", None),
        P("dp", None, "head", None),
        P("dp", None, "head"),
        P("dp", None),
    )
    out_specs = (P("dp", "head"), P("dp", None, "head", None), P("dp", None, "head"), P("dp", None))
    return jax.shard_map(body, mesh=mesh, in_specs=in_specs, out_specs=out_specs, check_vma=False)
```

```python
import math

import jax
import jax.numpy as jnp
from jax import lax
from jax.experimental import pallas as pl
from jax.experimental.pallas import tpu as pltpu
from jax.sharding import PartitionSpec as P

H = 8
DK = 256
DV = 512
EPSILON = 1e-06
F32 = jnp.float32
BF16 = jnp.bfloat16
STATS = 8


def exchange(pieces):
    return lax.all_to_all(pieces, "head", 0, 0, tiled=True)


def dot_last(left, right):
    return lax.dot_general(left, right, (((1,), (1,)), ((), ())), preferred_element_type=F32)


def dot(left, right):
    return jnp.dot(left, right, preferred_element_type=F32)


def column(row):
    n = row.shape[1]
    at_row = lax.broadcasted_iota(jnp.int32, (n, n), 0)
    at_col = lax.broadcasted_iota(jnp.int32, (n, n), 1)
    return jnp.sum(jnp.where(at_row == at_col, row, 0.0), axis=1, keepdims=True)


def split_hi_lo(value):
    high = value.astype(BF16).astype(F32)
    return high, value - high


def fetch(sources, targets, sems):
    copies = [pltpu.make_async_copy(s, t, sems.at[i]) for i, (s, t) in enumerate(zip(sources, targets))]
    for copy in copies:
        copy.start()
    return copies


def project_kernel(
    x_ref, gain_hbm, wi_hbm, wf_hbm, bi_hbm, bf_hbm, nrm_hbm, stab_hbm, wq_hbm, wk_hbm, mem_hbm,
    out_ref, xn_ref, nrm_out_ref, stab_out_ref, fg_ref, ig_ref, f_rows_ref, ik_rows_ref,
    stats_ref, gain_ref, wi_ref, wf_ref, bi_ref, bf_ref, nrm_ref, stab_ref, wq_ref, wk_ref, mem_ref, sems,
):
    sources = (gain_hbm, wi_hbm, wf_hbm, bi_hbm, bf_hbm, nrm_hbm, stab_hbm, wq_hbm, wk_hbm, mem_hbm)
    targets = (gain_ref, wi_ref, wf_ref, bi_ref, bf_ref, nrm_ref, stab_ref, wq_ref, wk_ref, mem_ref)
    copies = fetch(sources, targets, sems)
    pieces, batch, width = x_ref.shape
    rows = wq_ref.shape[0] // H
    total = jnp.zeros((batch, width), F32)
    for j in range(pieces):
        x = x_ref[j].astype(F32)
        total = total + x * x
    mean = jnp.sum(total, axis=1, keepdims=True) / (pieces * width)
    scale = lax.rsqrt(mean + EPSILON)
    stats_ref[...] = jnp.zeros(stats_ref.shape, F32)
    copies[0].wait()
    for j in range(pieces):
        cut = slice(j * width, (j + 1) * width)
        xn_ref[:, cut] = (x_ref[j].astype(F32) * scale * gain_ref[:, cut]).astype(BF16)
    x_norm = xn_ref[...]

    for copy in copies[1:7]:
        copy.wait()
    input_pre = dot_last(wi_ref[...], x_norm) + column(bi_ref[...])
    forget_pre = dot_last(wf_ref[...], x_norm) + column(bf_ref[...])
    log_forget = jnp.minimum(forget_pre, 0.0) - jnp.log1p(jnp.exp(-jnp.abs(forget_pre)))
    kept = log_forget + stab_ref[...]
    stab_new = jnp.maximum(kept, input_pre)
    input_gate = jnp.exp(input_pre - stab_new)
    forget_gate = jnp.exp(kept - stab_new)
    stab_out_ref[...] = stab_new
    fg_ref[...] = forget_gate
    ig_ref[...] = input_gate
    copies[7].wait()
    query = dot_last(x_norm, wq_ref[...])
    query_t = dot_last(wq_ref[...], x_norm)
    copies[8].wait()
    key_t = dot_last(wk_ref[...], x_norm) / math.sqrt(DK)

    for h in range(H):
        part = slice(h * rows, (h + 1) * rows)
        key_h = key_t[part]
        query_h = query_t[part]
        f_h = jnp.broadcast_to(forget_gate[h : h + 1], (rows, batch))
        ik_h = input_gate[h : h + 1] * key_h
        norm_h = f_h * nrm_ref[part] + ik_h
        nrm_out_ref[part] = norm_h
        f_rows_ref[part] = f_h
        ik_rows_ref[part] = ik_h
        norm_query = jnp.sum(norm_h * query_h, axis=0, keepdims=True)
        key_query = jnp.sum(key_h * query_h, axis=0, keepdims=True)
        kinds = (*split_hi_lo(norm_query), *split_hi_lo(key_query))
        for k, kind in enumerate(kinds):
            stats_ref[h, k : k + 1, :batch] = kind

    spread = batch * rows
    high, low = split_hi_lo(query)
    both = jnp.concatenate([high, low], axis=0).astype(BF16)
    at_k = lax.broadcasted_iota(jnp.int32, (rows, spread), 0)
    at_n = lax.broadcasted_iota(jnp.int32, (rows, spread), 1)
    repeat = jnp.where(at_n % rows == at_k, 1.0, 0.0).astype(BF16)
    own_b = lax.broadcasted_iota(jnp.int32, (2 * batch, spread), 0) % batch
    own_n = lax.broadcasted_iota(jnp.int32, (2 * batch, spread), 1) // rows
    own = own_b == own_n
    share = pieces // H
    copies[9].wait()
    for h in range(H):
        wide = dot(both[:, h * rows : (h + 1) * rows], repeat)
        left = jnp.where(own, wide, 0.0).astype(BF16)
        memory = mem_ref[:, h].astype(F32).reshape(spread, share * width).astype(BF16)
        product = dot(left, memory)
        numer = (product[:batch] + product[batch:]).astype(BF16)
        stats = stats_ref[h].astype(BF16)
        for c in range(share):
            out_ref[h * share + c, :batch] = numer[:, c * width : (c + 1) * width]
            out_ref[h * share + c, batch:] = stats


def gate_kernel(
    xn_ref, fg_ref, ig_ref, stab_ref, wv_hbm, wg_hbm,
    values_ref, sum_scale_ref, own_ref, floor_ref,
    wv_ref, wg_ref, sems,
):
    copies = fetch((wv_hbm, wg_hbm), (wv_ref, wg_ref), sems)
    head = lax.axis_index("head") * xn_ref.shape[1] // lax.axis_size("head") // DV
    pick = lambda ref: column(ref[pl.ds(head, 1), :])
    scales = [pick(ref) for ref in (fg_ref, ig_ref, stab_ref)]
    floor_ref[...] = jnp.broadcast_to(jnp.exp(-scales[2]), floor_ref.shape)
    x_norm = xn_ref[...]
    copies[0].wait()
    value = dot(x_norm, wv_ref[...]).astype(BF16)
    for j in range(values_ref.shape[0]):
        values_ref[j] = value
    copies[1].wait()
    gate = jax.nn.sigmoid(dot(x_norm, wg_ref[...]))
    sum_scale_ref[...] = gate * scales[0]
    own_ref[...] = gate * scales[1] * value.astype(F32)


def output_kernel(in_ref, sum_scale_ref, own_ref, floor_ref, wo_ref, out_ref):
    pieces, batch, width = out_ref.shape
    total = jnp.zeros(in_ref.shape[1:], F32)
    for j in range(pieces):
        total = total + in_ref[j].astype(F32)
    norm_query = column(total[batch : batch + 1, :batch] + total[batch + 1 : batch + 2, :batch])
    key_query = column(total[batch + 2 : batch + 3, :batch] + total[batch + 3 : batch + 4, :batch])
    numer = sum_scale_ref[...] * total[:batch] + own_ref[...] * key_query
    hidden = (numer / jnp.maximum(jnp.abs(norm_query), floor_ref[...])).astype(BF16)
    for j in range(pieces):
        out_ref[j] = dot(hidden, wo_ref[:, j * width : (j + 1) * width]).astype(BF16)


def memory_kernel(mem_ref, value_ref, f_rows_ref, ik_rows_ref, out_ref, wide_ref):
    pieces, batch, width = value_ref.shape
    share = pieces // H
    rows = mem_ref.shape[2]
    for j in range(pieces):
        cut = slice((j % share) * width, (j % share + 1) * width)
        wide_ref[j // share, :, cut] = value_ref[j].astype(F32)

    def one_head(h, carry):
        at = pl.multiple_of(h * rows, rows)
        f_rows = f_rows_ref[pl.ds(at, rows), :]
        ik_rows = ik_rows_ref[pl.ds(at, rows), :]
        for b in range(batch):
            kept = f_rows[:, b : b + 1] * mem_ref[b, h].astype(F32)
            out_ref[b, h] = (kept + ik_rows[:, b : b + 1] * wide_ref[h, b : b + 1, :]).astype(BF16)
        return carry

    lax.fori_loop(0, H, one_head, 0)


def finish_kernel(in_ref, residual_ref, out_ref):
    total = residual_ref[...]
    acc = in_ref[0].astype(F32)
    for j in range(1, in_ref.shape[0]):
        acc = acc + in_ref[j].astype(F32)
    out_ref[...] = total + acc


def call(kernel, outs, n_in, n_hbm=0, scratch=(), flops=1_000_000):
    return pl.pallas_call(
        kernel,
        out_shape=[jax.ShapeDtypeStruct(*out) for out in outs],
        in_specs=[pl.BlockSpec(memory_space=pltpu.VMEM)] * n_in
        + [pl.BlockSpec(memory_space=pltpu.HBM)] * n_hbm,
        out_specs=[pl.BlockSpec(memory_space=pltpu.VMEM)] * len(outs),
        scratch_shapes=list(scratch),
        compiler_params=pltpu.CompilerParams(vmem_limit_bytes=16 * 2**20),
        cost_estimate=pl.CostEstimate(flops=flops, bytes_accessed=2_000_000, transcendentals=0),
    )


def fetched(*arrays):
    return [pltpu.VMEM(a.shape, a.dtype) for a in arrays] + [pltpu.SemaphoreType.DMA((len(arrays),))]


def in_hbm(*arrays):
    return [pltpu.with_memory_space_constraint(a, pltpu.HBM) for a in arrays]


def body(
    residual,
    norm_gain,
    w_query,
    w_key,
    w_value,
    w_gate,
    w_input,
    w_forget,
    b_input,
    b_forget,
    w_out,
    memory,
    normalizer,
    stabilizer,
):
    count = lax.axis_size("head")
    batch, width = residual.shape
    rows = w_query.shape[1]
    features = count * width
    gathered = exchange(jnp.broadcast_to(residual.astype(BF16)[None], (count, batch, width)))

    piece = ((count, batch, width), BF16)
    sources = (
        norm_gain[None],
        w_input,
        w_forget,
        b_input[None],
        b_forget[None],
        normalizer.transpose(1, 2, 0).reshape(H * rows, batch),
        stabilizer.T,
        w_query.reshape(H * rows, features),
        w_key.reshape(H * rows, features),
        memory,
    )
    payload, x_norm, norm_new, stab_new, forget_gate, input_gate, f_rows, ik_rows = call(
        project_kernel,
        [
            ((count, batch + STATS, width), BF16),
            ((batch, features), BF16),
            ((H * rows, batch), F32),
            ((H, batch), F32),
            ((H, batch), F32),
            ((H, batch), F32),
            ((H * rows, batch), F32),
            ((H * rows, batch), F32),
        ],
        1,
        len(sources),
        scratch=[pltpu.VMEM((H, STATS, width), F32), *fetched(*sources)],
        flops=100_000_000,
    )(gathered, *in_hbm(*sources))
    arrived = exchange(payload)
    values, sum_scale, own, floor = call(
        gate_kernel,
        [piece] + [((batch, width), F32)] * 3,
        4,
        2,
        scratch=fetched(w_value, w_gate),
        flops=100_000_000,
    )(x_norm, forget_gate, input_gate, stab_new, *in_hbm(w_value, w_gate))
    value_heads = exchange(values)
    (branch,) = call(output_kernel, [piece], 5, flops=30_000_000)(
        arrived, sum_scale, own, floor, w_out
    )
    returned = exchange(branch)
    (mem_new,) = call(
        memory_kernel,
        [(memory.shape, BF16)],
        4,
        scratch=[pltpu.VMEM((H, batch, DV), F32)],
        flops=100_000_000,
    )(memory, value_heads, f_rows, ik_rows)
    (res_out,) = call(finish_kernel, [((batch, width), F32)], 2)(returned, residual)
    norm_out = norm_new.reshape(H, rows, batch).transpose(2, 0, 1)
    return res_out, mem_new, norm_out, stab_new.T


def solution(mesh):
    in_specs = (
        P("dp", "head"),
        P(),
        P(None, "head", None),
        P(None, "head", None),
        P(None, "head"),
        P(None, "head"),
        P(),
        P(),
        P(),
        P(),
        P("head", None),
        P("dp", None, "head", None),
        P("dp", None, "head"),
        P("dp", None),
    )
    out_specs = (P("dp", "head"), P("dp", None, "head", None), P("dp", None, "head"), P("dp", None))
    return jax.shard_map(body, mesh=mesh, in_specs=in_specs, out_specs=out_specs, check_vma=False)
```

```python
import math

import jax
import jax.numpy as jnp
from jax import lax
from jax.experimental import pallas as pl
from jax.experimental.pallas import tpu as pltpu
from jax.sharding import PartitionSpec as P

H = 8
DK = 256
DV = 512
EPSILON = 1e-06
F32 = jnp.float32
BF16 = jnp.bfloat16
STATS = 8


def exchange(pieces):
    return lax.all_to_all(pieces, "head", 0, 0, tiled=True)


def dot_last(left, right):
    return lax.dot_general(left, right, (((1,), (1,)), ((), ())), preferred_element_type=F32)


def dot(left, right):
    return jnp.dot(left, right, preferred_element_type=F32)


def column(row):
    n = row.shape[1]
    at_row = lax.broadcasted_iota(jnp.int32, (n, n), 0)
    at_col = lax.broadcasted_iota(jnp.int32, (n, n), 1)
    return jnp.sum(jnp.where(at_row == at_col, row, 0.0), axis=1, keepdims=True)


def split_hi_lo(value):
    high = value.astype(BF16).astype(F32)
    return high, value - high


def fetch(sources, targets, sems):
    copies = [pltpu.make_async_copy(s, t, sems.at[i]) for i, (s, t) in enumerate(zip(sources, targets))]
    for copy in copies:
        copy.start()
    return copies


def prefetch_kernel(
    gain_hbm, wi_hbm, wf_hbm, bi_hbm, bf_hbm, nrm_hbm, stab_hbm, wq_hbm, wk_hbm, mem_hbm,
    gain_ref, wi_ref, wf_ref, bi_ref, bf_ref, nrm_ref, stab_ref, wq_ref, wk_ref, by_head_ref,
    mem_ref, sems,
):
    sources = (mem_hbm, gain_hbm, wi_hbm, wf_hbm, bi_hbm, bf_hbm, nrm_hbm, stab_hbm, wq_hbm, wk_hbm)
    targets = (mem_ref, gain_ref, wi_ref, wf_ref, bi_ref, bf_ref, nrm_ref, stab_ref, wq_ref, wk_ref)
    copies = fetch(sources, targets, sems)
    copies[0].wait()
    for h in range(H):
        by_head_ref[h] = mem_ref[:, h].astype(F32).reshape(by_head_ref.shape[1:]).astype(BF16)
    for copy in copies[1:]:
        copy.wait()


def project_kernel(
    x_ref, gain_ref, wi_ref, wf_ref, bi_ref, bf_ref, nrm_ref, stab_ref, wq_ref, wk_ref, by_head_ref,
    wv_hbm, wg_hbm,
    out_ref, nrm_out_ref, stab_out_ref, f_rows_ref, ik_rows_ref, sum_scale_ref, own_ref, floor_ref,
    xn_ref, tail_ref, fg_ref, ig_ref, wv_ref, wg_ref, sems,
):
    copies = fetch((wv_hbm, wg_hbm), (wv_ref, wg_ref), sems)
    pieces, batch, width = x_ref.shape
    half = batch // 2
    rows = wq_ref.shape[0] // H
    total = jnp.zeros((batch, width), F32)
    for j in range(pieces):
        x = x_ref[j].astype(F32)
        total = total + x * x
    mean = jnp.sum(total, axis=1, keepdims=True) / (pieces * width)
    scale = lax.rsqrt(mean + EPSILON)
    tail_ref[...] = jnp.zeros(tail_ref.shape, F32)
    for j in range(pieces):
        cut = slice(j * width, (j + 1) * width)
        xn_ref[:, cut] = (x_ref[j].astype(F32) * scale * gain_ref[:, cut]).astype(BF16)
    x_norm = xn_ref[...]

    query = dot_last(x_norm, wq_ref[...])
    query_t = dot_last(wq_ref[...], x_norm)
    key_t = dot_last(wk_ref[...], x_norm) / math.sqrt(DK)
    input_pre = dot_last(wi_ref[...], x_norm) + column(bi_ref[...])
    forget_pre = dot_last(wf_ref[...], x_norm) + column(bf_ref[...])
    log_forget = jnp.minimum(forget_pre, 0.0) - jnp.log1p(jnp.exp(-jnp.abs(forget_pre)))
    kept = log_forget + stab_ref[...]
    stab_new = jnp.maximum(kept, input_pre)
    input_gate = jnp.exp(input_pre - stab_new)
    forget_gate = jnp.exp(kept - stab_new)
    stab_out_ref[...] = stab_new
    fg_ref[...] = forget_gate
    ig_ref[...] = input_gate

    for h in range(H):
        part = slice(h * rows, (h + 1) * rows)
        key_h = key_t[part]
        query_h = query_t[part]
        f_h = jnp.broadcast_to(forget_gate[h : h + 1], (rows, batch))
        ik_h = input_gate[h : h + 1] * key_h
        norm_h = f_h * nrm_ref[part] + ik_h
        nrm_out_ref[part] = norm_h
        f_rows_ref[part] = f_h
        ik_rows_ref[part] = ik_h
        norm_query = jnp.sum(norm_h * query_h, axis=0, keepdims=True)
        key_query = jnp.sum(key_h * query_h, axis=0, keepdims=True)
        kinds = (*split_hi_lo(norm_query), *split_hi_lo(key_query))
        for k, kind in enumerate(kinds):
            for core in range(2):
                tail_ref[core, h, 4 + k : 5 + k, :batch] = kind

    spread = batch * rows
    high, low = split_hi_lo(query)
    both = jnp.concatenate([high, low], axis=0).astype(BF16)
    at_k = lax.broadcasted_iota(jnp.int32, (rows, spread), 0)
    at_n = lax.broadcasted_iota(jnp.int32, (rows, spread), 1)
    repeat = jnp.where(at_n % rows == at_k, 1.0, 0.0).astype(BF16)
    own_b = lax.broadcasted_iota(jnp.int32, (2 * batch, spread), 0) % batch
    own_n = lax.broadcasted_iota(jnp.int32, (2 * batch, spread), 1) // rows
    own = own_b == own_n
    share = pieces // H
    for h in range(H):
        wide = dot(both[:, h * rows : (h + 1) * rows], repeat)
        left = jnp.where(own, wide, 0.0).astype(BF16)
        product = dot(left, by_head_ref[h])
        numer = (product[:batch] + product[batch:]).astype(BF16)
        for c in range(share):
            out_ref[h * share + c, :batch] = numer[:, c * width : (c + 1) * width]

    copies[0].wait()
    value = dot(x_norm, wv_ref[...])
    for core in range(2):
        first = value[core * half : core * half + 8].astype(BF16)
        rest = value[core * half + 8 : (core + 1) * half]
        for h in range(H):
            tail_ref[core, h, :4] = rest
        for j in range(core, pieces, 2):
            out_ref[j, batch : batch + 8] = first
            out_ref[j, batch + 8 :] = tail_ref[core, j // share].astype(BF16)

    head = lax.axis_index("head") * width // DV
    pick = lambda ref: column(ref[pl.ds(head, 1), :])
    copies[1].wait()
    gate = jax.nn.sigmoid(dot(x_norm, wg_ref[...]))
    sum_scale_ref[...] = gate * pick(fg_ref)
    own_ref[...] = gate * (pick(ig_ref) * value.astype(BF16).astype(F32))
    floor_ref[...] = jnp.broadcast_to(jnp.exp(-pick(stab_out_ref)), floor_ref.shape)


def output_kernel(in_ref, sum_scale_ref, own_ref, floor_ref, wo_ref, out_ref):
    pieces, batch, width = out_ref.shape
    total = in_ref[0, :batch].astype(F32)
    tail = in_ref[0, batch + 8 :].astype(F32)
    for j in range(1, pieces):
        total = total + in_ref[j, :batch].astype(F32)
        tail = tail + in_ref[j, batch + 8 :].astype(F32)
    norm_query = column(tail[4:5, :batch] + tail[5:6, :batch])
    key_query = column(tail[6:7, :batch] + tail[7:8, :batch])
    numer = sum_scale_ref[...] * total + own_ref[...] * key_query
    hidden = (numer / jnp.maximum(jnp.abs(norm_query), floor_ref[...])).astype(BF16)
    for j in range(pieces):
        out_ref[j] = dot(hidden, wo_ref[:, j * width : (j + 1) * width]).astype(BF16)


def memory_kernel(f_rows_ref, ik_rows_ref, mine_ref, other_ref, mem_ref, out_ref, wide_ref):
    pieces = mine_ref.shape[0]
    batch, _, rows, _ = mem_ref.shape
    width = mine_ref.shape[2]
    half = batch // 2
    share = pieces // H
    even = lax.axis_index("head") % 2 == 0
    for j in range(pieces):
        cut = slice((j % share) * width, (j % share + 1) * width)
        mine = mine_ref[j, batch : batch + 16].astype(F32)[:half]
        other = other_ref[j].astype(F32)[:half]
        wide_ref[j // share, :half, cut] = jnp.where(even, mine, other)
        wide_ref[j // share, half:, cut] = jnp.where(even, other, mine)

    def one_head(h, carry):
        at = pl.multiple_of(h * rows, rows)
        f_rows = f_rows_ref[pl.ds(at, rows), :]
        ik_rows = ik_rows_ref[pl.ds(at, rows), :]
        for b in range(batch):
            kept = f_rows[:, b : b + 1] * mem_ref[b, h].astype(F32)
            out_ref[b, h] = (kept + ik_rows[:, b : b + 1] * wide_ref[h, b : b + 1, :]).astype(BF16)
        return carry

    lax.fori_loop(0, H, one_head, 0)


def finish_kernel(in_ref, residual_ref, out_ref):
    total = residual_ref[...]
    acc = in_ref[0].astype(F32)
    for j in range(1, in_ref.shape[0]):
        acc = acc + in_ref[j].astype(F32)
    out_ref[...] = total + acc


def call(kernel, outs, n_in, n_hbm=0, scratch=(), flops=1_000_000):
    return pl.pallas_call(
        kernel,
        out_shape=[jax.ShapeDtypeStruct(*out) for out in outs],
        in_specs=[pl.BlockSpec(memory_space=pltpu.VMEM)] * n_in
        + [pl.BlockSpec(memory_space=pltpu.HBM)] * n_hbm,
        out_specs=[pl.BlockSpec(memory_space=pltpu.VMEM)] * len(outs),
        scratch_shapes=list(scratch),
        compiler_params=pltpu.CompilerParams(vmem_limit_bytes=16 * 2**20),
        cost_estimate=pl.CostEstimate(flops=flops, bytes_accessed=2_000_000, transcendentals=0),
    )


def fetched(*arrays):
    return [pltpu.VMEM(a.shape, a.dtype) for a in arrays] + [pltpu.SemaphoreType.DMA((len(arrays),))]


def in_hbm(*arrays):
    return [pltpu.with_memory_space_constraint(a, pltpu.HBM) for a in arrays]


def body(
    residual,
    norm_gain,
    w_query,
    w_key,
    w_value,
    w_gate,
    w_input,
    w_forget,
    b_input,
    b_forget,
    w_out,
    memory,
    normalizer,
    stabilizer,
):
    count = lax.axis_size("head")
    batch, width = residual.shape
    rows = w_query.shape[1]
    features = count * width
    gathered = exchange(jnp.broadcast_to(residual.astype(BF16)[None], (count, batch, width)))

    piece = ((count, batch, width), BF16)
    sources = (
        norm_gain[None],
        w_input,
        w_forget,
        b_input[None],
        b_forget[None],
        normalizer.transpose(1, 2, 0).reshape(H * rows, batch),
        stabilizer.T,
        w_query.reshape(H * rows, features),
        w_key.reshape(H * rows, features),
    )
    by_head = ((H, batch * rows, DV), BF16)
    with jax.named_scope("prefetch"):
        ready = call(
            prefetch_kernel,
            [*((a.shape, a.dtype) for a in sources), by_head],
            0,
            len(sources) + 1,
            scratch=[
                pltpu.VMEM(memory.shape, memory.dtype),
                pltpu.SemaphoreType.DMA((len(sources) + 1,)),
            ],
            flops=100_000_000,
        )(*in_hbm(*sources, memory))
    payload, norm_new, stab_new, f_rows, ik_rows, sum_scale, own, floor = call(
        project_kernel,
        [
            ((count, batch + batch // 2 + 4, width), BF16),
            ((H * rows, batch), F32),
            ((H, batch), F32),
            ((H * rows, batch), F32),
            ((H * rows, batch), F32),
            ((batch, width), F32),
            ((batch, width), F32),
            ((batch, width), F32),
        ],
        1 + len(ready),
        2,
        scratch=[
            pltpu.VMEM((batch, features), BF16),
            pltpu.VMEM((2, H, 8, width), F32),
            pltpu.VMEM((H, batch), F32),
            pltpu.VMEM((H, batch), F32),
            *fetched(w_value, w_gate),
        ],
        flops=100_000_000,
    )(gathered, *ready, *in_hbm(w_value, w_gate))
    arrived = exchange(payload)
    (branch,) = call(output_kernel, [piece], 5, flops=30_000_000)(
        arrived, sum_scale, own, floor, w_out
    )
    returned = exchange(branch)
    with jax.named_scope("swap"):
        other = lax.ppermute(arrived[:, batch:], "head", [(i, i ^ 1) for i in range(count)])
    (mem_new,) = call(
        memory_kernel,
        [(memory.shape, BF16)],
        5,
        scratch=[pltpu.VMEM((H, batch, DV), F32)],
        flops=100_000_000,
    )(f_rows, ik_rows, arrived, other, memory)
    (res_out,) = call(finish_kernel, [((batch, width), F32)], 2)(returned, residual)
    norm_out = norm_new.reshape(H, rows, batch).transpose(2, 0, 1)
    return res_out, mem_new, norm_out, stab_new.T


def solution(mesh):
    in_specs = (
        P("dp", "head"),
        P(),
        P(None, "head", None),
        P(None, "head", None),
        P(None, "head"),
        P(None, "head"),
        P(),
        P(),
        P(),
        P(),
        P("head", None),
        P("dp", None, "head", None),
        P("dp", None, "head"),
        P("dp", None),
    )
    out_specs = (P("dp", "head"), P("dp", None, "head", None), P("dp", None, "head"), P("dp", None))
    return jax.shard_map(body, mesh=mesh, in_specs=in_specs, out_specs=out_specs, check_vma=False)
```

```python
import math

import jax
import jax.numpy as jnp
from jax import lax
from jax.experimental import pallas as pl
from jax.experimental.pallas import tpu as pltpu
from jax.sharding import PartitionSpec as P

H = 8
DK = 256
DV = 512
EPSILON = 1e-06
F32 = jnp.float32
BF16 = jnp.bfloat16
STATS = 8


SPREAD_FLOPS = 10_000_000_000


def exchange(pieces):
    return lax.all_to_all(pieces, "head", 0, 0, tiled=True)


def dot_last(left, right):
    return lax.dot_general(left, right, (((1,), (1,)), ((), ())), preferred_element_type=F32)


def dot(left, right):
    return jnp.dot(left, right, preferred_element_type=F32)


def column(row):
    n = row.shape[1]
    at_row = lax.broadcasted_iota(jnp.int32, (n, n), 0)
    at_col = lax.broadcasted_iota(jnp.int32, (n, n), 1)
    return jnp.sum(jnp.where(at_row == at_col, row, 0.0), axis=1, keepdims=True)


def split_hi_lo(value):
    high = value.astype(BF16).astype(F32)
    return high, value - high


def spread_kernel(in_ref, out_ref):
    value = in_ref[...]
    for j in range(out_ref.shape[0]):
        out_ref[j] = value


def project_kernel(
    x_ref, gain_ref, wi_ref, wf_ref, bi_ref, bf_ref, nrm_ref, stab_ref, wq_ref, wk_ref, wv_ref, wg_ref, mem_ref,
    out_ref, nrm_out_ref, stab_out_ref, f_rows_ref, ik_rows_ref, sum_scale_ref, own_ref, floor_ref,
    xn_ref, tail_ref, fg_ref, ig_ref,
):
    pieces, batch, width = x_ref.shape
    half = batch // 2
    rows = wq_ref.shape[0] // H
    total = jnp.zeros((batch, width), F32)
    for j in range(pieces):
        x = x_ref[j].astype(F32)
        total = total + x * x
    mean = jnp.sum(total, axis=1, keepdims=True) / (pieces * width)
    scale = lax.rsqrt(mean + EPSILON)
    tail_ref[...] = jnp.zeros(tail_ref.shape, F32)
    for j in range(pieces):
        cut = slice(j * width, (j + 1) * width)
        xn_ref[:, cut] = (x_ref[j].astype(F32) * scale * gain_ref[:, cut]).astype(BF16)
    x_norm = xn_ref[...]

    query = dot_last(x_norm, wq_ref[...])
    query_t = dot_last(wq_ref[...], x_norm)
    key_t = dot_last(wk_ref[...], x_norm) / math.sqrt(DK)
    input_pre = dot_last(wi_ref[...], x_norm) + column(bi_ref[...])
    forget_pre = dot_last(wf_ref[...], x_norm) + column(bf_ref[...])
    log_forget = jnp.minimum(forget_pre, 0.0) - jnp.log1p(jnp.exp(-jnp.abs(forget_pre)))
    kept = log_forget + stab_ref[...]
    stab_new = jnp.maximum(kept, input_pre)
    input_gate = jnp.exp(input_pre - stab_new)
    forget_gate = jnp.exp(kept - stab_new)
    stab_out_ref[...] = stab_new
    fg_ref[...] = forget_gate
    ig_ref[...] = input_gate

    for h in range(H):
        part = slice(h * rows, (h + 1) * rows)
        key_h = key_t[part]
        query_h = query_t[part]
        f_h = jnp.broadcast_to(forget_gate[h : h + 1], (rows, batch))
        ik_h = input_gate[h : h + 1] * key_h
        norm_h = f_h * nrm_ref[part] + ik_h
        nrm_out_ref[part] = norm_h
        f_rows_ref[part] = f_h
        ik_rows_ref[part] = ik_h
        norm_query = jnp.sum(norm_h * query_h, axis=0, keepdims=True)
        key_query = jnp.sum(key_h * query_h, axis=0, keepdims=True)
        kinds = (*split_hi_lo(norm_query), *split_hi_lo(key_query))
        for k, kind in enumerate(kinds):
            for core in range(2):
                tail_ref[core, h, 4 + k : 5 + k, :batch] = kind

    spread = batch * rows
    high, low = split_hi_lo(query)
    both = jnp.concatenate([high, low], axis=0).astype(BF16)
    at_k = lax.broadcasted_iota(jnp.int32, (rows, spread), 0)
    at_n = lax.broadcasted_iota(jnp.int32, (rows, spread), 1)
    repeat = jnp.where(at_n % rows == at_k, 1.0, 0.0).astype(BF16)
    own_b = lax.broadcasted_iota(jnp.int32, (2 * batch, spread), 0) % batch
    own_n = lax.broadcasted_iota(jnp.int32, (2 * batch, spread), 1) // rows
    own = own_b == own_n
    share = pieces // H
    for h in range(H):
        wide = dot(both[:, h * rows : (h + 1) * rows], repeat)
        left = jnp.where(own, wide, 0.0).astype(BF16)
        by_head = mem_ref[:, h].astype(F32).reshape(spread, share * width).astype(BF16)
        product = dot(left, by_head)
        numer = (product[:batch] + product[batch:]).astype(BF16)
        for c in range(share):
            out_ref[h * share + c, :batch] = numer[:, c * width : (c + 1) * width]

    value = dot(x_norm, wv_ref[...])
    for core in range(2):
        first = value[core * half : core * half + 8].astype(BF16)
        rest = value[core * half + 8 : (core + 1) * half]
        for h in range(H):
            tail_ref[core, h, :4] = rest
        for j in range(core, pieces, 2):
            out_ref[j, batch : batch + 8] = first
            out_ref[j, batch + 8 :] = tail_ref[core, j // share].astype(BF16)

    head = lax.axis_index("head") * width // DV
    pick = lambda ref: column(ref[pl.ds(head, 1), :])
    gate = jax.nn.sigmoid(dot(x_norm, wg_ref[...]))
    sum_scale_ref[...] = gate * pick(fg_ref)
    own_ref[...] = gate * (pick(ig_ref) * value.astype(BF16).astype(F32))
    floor_ref[...] = jnp.broadcast_to(jnp.exp(-pick(stab_out_ref)), floor_ref.shape)


def output_kernel(in_ref, sum_scale_ref, own_ref, floor_ref, wo_ref, out_ref):
    pieces, batch, width = out_ref.shape
    total = in_ref[0, :batch].astype(F32)
    tail = in_ref[0, batch + 8 :].astype(F32)
    for j in range(1, pieces):
        total = total + in_ref[j, :batch].astype(F32)
        tail = tail + in_ref[j, batch + 8 :].astype(F32)
    norm_query = column(tail[4:5, :batch] + tail[5:6, :batch])
    key_query = column(tail[6:7, :batch] + tail[7:8, :batch])
    numer = sum_scale_ref[...] * total + own_ref[...] * key_query
    hidden = (numer / jnp.maximum(jnp.abs(norm_query), floor_ref[...])).astype(BF16)
    for j in range(pieces):
        out_ref[j] = dot(hidden, wo_ref[:, j * width : (j + 1) * width]).astype(BF16)


def memory_kernel(
    f_rows_ref, ik_rows_ref, norm_ref, stab_ref, mine_ref, other_ref, mem_ref,
    out_ref, norm_out_ref, stab_out_ref, wide_ref,
):
    norm_out_ref[...] = norm_ref[...]
    stab_out_ref[...] = stab_ref[...]
    pieces = mine_ref.shape[0]
    batch, _, rows, _ = mem_ref.shape
    width = mine_ref.shape[2]
    half = batch // 2
    share = pieces // H
    even = lax.axis_index("head") % 2 == 0
    for j in range(pieces):
        cut = slice((j % share) * width, (j % share + 1) * width)
        mine = mine_ref[j, batch : batch + 16].astype(F32)[:half]
        other = other_ref[j].astype(F32)[:half]
        wide_ref[j // share, :half, cut] = jnp.where(even, mine, other)
        wide_ref[j // share, half:, cut] = jnp.where(even, other, mine)

    def one_head(h, carry):
        at = pl.multiple_of(h * rows, rows)
        f_rows = f_rows_ref[pl.ds(at, rows), :]
        ik_rows = ik_rows_ref[pl.ds(at, rows), :]
        for b in range(batch):
            kept = f_rows[:, b : b + 1] * mem_ref[b, h].astype(F32)
            out_ref[b, h] = (kept + ik_rows[:, b : b + 1] * wide_ref[h, b : b + 1, :]).astype(BF16)
        return carry

    lax.fori_loop(0, H, one_head, 0)


def finish_kernel(in_ref, residual_ref, out_ref):
    total = residual_ref[...]
    acc = in_ref[0].astype(F32)
    for j in range(1, in_ref.shape[0]):
        acc = acc + in_ref[j].astype(F32)
    out_ref[...] = total + acc


def call(kernel, outs, n_in, scratch=(), flops=1_000_000):
    return pl.pallas_call(
        kernel,
        out_shape=[jax.ShapeDtypeStruct(*out) for out in outs],
        in_specs=[pl.BlockSpec(memory_space=pltpu.VMEM)] * n_in,
        out_specs=[pl.BlockSpec(memory_space=pltpu.VMEM)] * len(outs),
        scratch_shapes=list(scratch),
        compiler_params=pltpu.CompilerParams(vmem_limit_bytes=16 * 2**20),
        cost_estimate=pl.CostEstimate(flops=flops, bytes_accessed=2_000_000, transcendentals=0),
    )


def body(
    residual,
    norm_gain,
    w_query,
    w_key,
    w_value,
    w_gate,
    w_input,
    w_forget,
    b_input,
    b_forget,
    w_out,
    memory,
    normalizer,
    stabilizer,
):
    count = lax.axis_size("head")
    batch, width = residual.shape
    rows = w_query.shape[1]
    features = count * width
    (pieces,) = call(spread_kernel, [((count, batch, width), BF16)], 1, flops=SPREAD_FLOPS)(
        residual.astype(BF16)
    )
    gathered = exchange(pieces)

    piece = ((count, batch, width), BF16)
    sources = (
        norm_gain[None],
        w_input,
        w_forget,
        b_input[None],
        b_forget[None],
        normalizer.transpose(1, 2, 0).reshape(H * rows, batch),
        stabilizer.T,
        w_query.reshape(H * rows, features),
        w_key.reshape(H * rows, features),
        w_value,
        w_gate,
        memory,
    )
    payload, norm_new, stab_new, f_rows, ik_rows, sum_scale, own, floor = call(
        project_kernel,
        [
            ((count, batch + batch // 2 + 4, width), BF16),
            ((H * rows, batch), F32),
            ((H, batch), F32),
            ((H * rows, batch), F32),
            ((H * rows, batch), F32),
            ((batch, width), F32),
            ((batch, width), F32),
            ((batch, width), F32),
        ],
        1 + len(sources),
        scratch=[
            pltpu.VMEM((batch, features), BF16),
            pltpu.VMEM((2, H, 8, width), F32),
            pltpu.VMEM((H, batch), F32),
            pltpu.VMEM((H, batch), F32),
        ],
        flops=100_000_000,
    )(gathered, *sources)
    arrived = exchange(payload)
    (branch,) = call(output_kernel, [piece], 5, flops=30_000_000)(
        arrived, sum_scale, own, floor, w_out
    )
    returned = exchange(branch)
    with jax.named_scope("swap"):
        other = lax.ppermute(arrived[:, batch:], "head", [(i, i ^ 1) for i in range(count)])
    mem_new, norm_out, stab_out = call(
        memory_kernel,
        [(memory.shape, BF16), ((H * rows, batch), F32), ((H, batch), F32)],
        7,
        scratch=[pltpu.VMEM((H, batch, DV), F32)],
        flops=100_000_000,
    )(f_rows, ik_rows, norm_new, stab_new, arrived, other, memory)
    (res_out,) = call(finish_kernel, [((batch, width), F32)], 2)(returned, residual)
    norm_out = norm_out.reshape(H, rows, batch).transpose(2, 0, 1)
    return res_out, mem_new, norm_out, stab_out.T


def solution(mesh):
    in_specs = (
        P("dp", "head"),
        P(),
        P(None, "head", None),
        P(None, "head", None),
        P(None, "head"),
        P(None, "head"),
        P(),
        P(),
        P(),
        P(),
        P("head", None),
        P("dp", None, "head", None),
        P("dp", None, "head"),
        P("dp", None),
    )
    out_specs = (P("dp", "head"), P("dp", None, "head", None), P("dp", None, "head"), P("dp", None))
    return jax.shard_map(body, mesh=mesh, in_specs=in_specs, out_specs=out_specs, check_vma=False)
```

```python
import math

import jax
import jax.numpy as jnp
import numpy as np
from jax import lax
from jax.experimental import pallas as pl
from jax.experimental.pallas import tpu as pltpu
from jax.sharding import PartitionSpec as P

H = 8
DK = 256
DV = 512
EPSILON = 1e-06
F32 = jnp.float32
BF16 = jnp.bfloat16
STATS = 8


SPREAD_FLOPS = 10_000_000_000


def exchange(pieces):
    return lax.all_to_all(pieces, "head", 0, 0, tiled=True)


def dot_last(left, right):
    return lax.dot_general(left, right, (((1,), (1,)), ((), ())), preferred_element_type=F32)


def dot(left, right):
    return jnp.dot(left, right, preferred_element_type=F32)


def column(row):
    n = row.shape[1]
    at_row = lax.broadcasted_iota(jnp.int32, (n, n), 0)
    at_col = lax.broadcasted_iota(jnp.int32, (n, n), 1)
    return jnp.sum(jnp.where(at_row == at_col, row, 0.0), axis=1, keepdims=True)


def split_hi_lo(value):
    high = value.astype(BF16).astype(F32)
    return high, value - high


def repeat_matrix(rows, batch):
    spread = batch * rows
    stride = -(-spread // 256) * 256
    col = np.arange(H * stride)
    source = col // stride * rows + col % rows
    hit = (np.arange(H * rows)[:, None] == source) & (col % stride < spread)
    return jnp.asarray(hit, BF16)


def spread_kernel(in_ref, out_ref):
    value = in_ref[...]
    for j in range(out_ref.shape[0]):
        out_ref[j] = value


def project_kernel(
    x_ref, gain_ref, wi_ref, wf_ref, bi_ref, bf_ref, nrm_ref, stab_ref, wq_ref, wk_ref, wv_ref, wg_ref, mem_ref,
    repeat_ref,
    out_ref, nrm_out_ref, stab_out_ref, f_rows_ref, ik_rows_ref, sum_scale_ref, own_ref, floor_ref,
    xn_ref, tail_ref, fg_ref, ig_ref,
):
    pieces, batch, width = x_ref.shape
    half = batch // 2
    rows = wq_ref.shape[0] // H
    total = jnp.zeros((batch, width), F32)
    for j in range(pieces):
        x = x_ref[j].astype(F32)
        total = total + x * x
    mean = jnp.sum(total, axis=1, keepdims=True) / (pieces * width)
    scale = lax.rsqrt(mean + EPSILON)
    tail_ref[...] = jnp.zeros(tail_ref.shape, F32)
    for j in range(pieces):
        cut = slice(j * width, (j + 1) * width)
        xn_ref[:, cut] = (x_ref[j].astype(F32) * scale * gain_ref[:, cut]).astype(BF16)
    x_norm = xn_ref[...]

    left = jnp.concatenate([wq_ref[...], wk_ref[...], wi_ref[...], wf_ref[...]], axis=0)
    mixed = dot_last(left, x_norm)
    query_t = mixed[: H * rows]
    key_t = mixed[H * rows : 2 * H * rows] / math.sqrt(DK)
    input_pre = mixed[2 * H * rows : 2 * H * rows + H] + column(bi_ref[...])
    forget_pre = mixed[2 * H * rows + H :] + column(bf_ref[...])
    log_forget = jnp.minimum(forget_pre, 0.0) - jnp.log1p(jnp.exp(-jnp.abs(forget_pre)))
    kept = log_forget + stab_ref[...]
    stab_new = jnp.maximum(kept, input_pre)
    input_gate = jnp.exp(input_pre - stab_new)
    forget_gate = jnp.exp(kept - stab_new)
    stab_out_ref[...] = stab_new
    fg_ref[...] = forget_gate
    ig_ref[...] = input_gate

    for h in range(H):
        part = slice(h * rows, (h + 1) * rows)
        key_h = key_t[part]
        query_h = query_t[part]
        f_h = jnp.broadcast_to(forget_gate[h : h + 1], (rows, batch))
        ik_h = input_gate[h : h + 1] * key_h
        norm_h = f_h * nrm_ref[part] + ik_h
        nrm_out_ref[part] = norm_h
        f_rows_ref[part] = f_h
        ik_rows_ref[part] = ik_h
        norm_query = jnp.sum(norm_h * query_h, axis=0, keepdims=True)
        key_query = jnp.sum(key_h * query_h, axis=0, keepdims=True)
        kinds = (*split_hi_lo(norm_query), *split_hi_lo(key_query))
        for k, kind in enumerate(kinds):
            for core in range(2):
                tail_ref[core, h, 4 + k : 5 + k, :batch] = kind

    spread = batch * rows
    high, low = split_hi_lo(query_t.T)
    both = jnp.concatenate([high, low], axis=0).astype(BF16)
    stride = repeat_ref.shape[1] // H
    wide = dot(both, repeat_ref[...])
    own_b = lax.broadcasted_iota(jnp.int32, (2 * batch, spread), 0) % batch
    own_n = lax.broadcasted_iota(jnp.int32, (2 * batch, spread), 1) // rows
    own = own_b == own_n
    share = pieces // H
    for h in range(H):
        left = jnp.where(own, wide[:, h * stride : h * stride + spread], 0.0).astype(BF16)
        by_head = mem_ref[:, h].astype(F32).reshape(spread, share * width).astype(BF16)
        product = dot(left, by_head)
        numer = (product[:batch] + product[batch:]).astype(BF16)
        for c in range(share):
            out_ref[h * share + c, :batch] = numer[:, c * width : (c + 1) * width]

    value_gate = dot(x_norm, jnp.concatenate([wv_ref[...], wg_ref[...]], axis=1))
    value = value_gate[:, :width]
    for core in range(2):
        first = value[core * half : core * half + 8].astype(BF16)
        rest = value[core * half + 8 : (core + 1) * half]
        for h in range(H):
            tail_ref[core, h, :4] = rest
        for j in range(core, pieces, 2):
            out_ref[j, batch : batch + 8] = first
            out_ref[j, batch + 8 :] = tail_ref[core, j // share].astype(BF16)

    head = lax.axis_index("head") * width // DV
    pick = lambda ref: column(ref[pl.ds(head, 1), :])
    gate = jax.nn.sigmoid(value_gate[:, width:])
    sum_scale_ref[...] = gate * pick(fg_ref)
    own_ref[...] = gate * (pick(ig_ref) * value.astype(BF16).astype(F32))
    floor_ref[...] = jnp.broadcast_to(jnp.exp(-pick(stab_out_ref)), floor_ref.shape)


def output_kernel(in_ref, sum_scale_ref, own_ref, floor_ref, wo_ref, out_ref):
    pieces, batch, width = out_ref.shape
    total = in_ref[0, :batch].astype(F32)
    tail = in_ref[0, batch + 8 :].astype(F32)
    for j in range(1, pieces):
        total = total + in_ref[j, :batch].astype(F32)
        tail = tail + in_ref[j, batch + 8 :].astype(F32)
    norm_query = column(tail[4:5, :batch] + tail[5:6, :batch])
    key_query = column(tail[6:7, :batch] + tail[7:8, :batch])
    numer = sum_scale_ref[...] * total + own_ref[...] * key_query
    hidden = (numer / jnp.maximum(jnp.abs(norm_query), floor_ref[...])).astype(BF16)
    for j in range(0, pieces, 2):
        pair = dot(hidden, wo_ref[:, j * width : (j + 2) * width]).astype(BF16)
        out_ref[j] = pair[:, :width]
        out_ref[j + 1] = pair[:, width:]


def memory_kernel(
    f_rows_ref, ik_rows_ref, norm_ref, stab_ref, mine_ref, other_ref, mem_ref,
    out_ref, norm_out_ref, stab_out_ref, wide_ref,
):
    norm_out_ref[...] = norm_ref[...]
    stab_out_ref[...] = stab_ref[...]
    pieces = mine_ref.shape[0]
    batch, _, rows, _ = mem_ref.shape
    width = mine_ref.shape[2]
    half = batch // 2
    share = pieces // H
    even = lax.axis_index("head") % 2 == 0
    for j in range(pieces):
        cut = slice((j % share) * width, (j % share + 1) * width)
        mine = mine_ref[j, batch : batch + 16].astype(F32)[:half]
        other = other_ref[j].astype(F32)[:half]
        wide_ref[j // share, :half, cut] = jnp.where(even, mine, other)
        wide_ref[j // share, half:, cut] = jnp.where(even, other, mine)

    def one_head(h, carry):
        at = pl.multiple_of(h * rows, rows)
        f_rows = f_rows_ref[pl.ds(at, rows), :]
        ik_rows = ik_rows_ref[pl.ds(at, rows), :]
        for b in range(batch):
            kept = f_rows[:, b : b + 1] * mem_ref[b, h].astype(F32)
            out_ref[b, h] = (kept + ik_rows[:, b : b + 1] * wide_ref[h, b : b + 1, :]).astype(BF16)
        return carry

    lax.fori_loop(0, H, one_head, 0)


def finish_kernel(in_ref, residual_ref, out_ref):
    total = residual_ref[...]
    acc = in_ref[0].astype(F32)
    for j in range(1, in_ref.shape[0]):
        acc = acc + in_ref[j].astype(F32)
    out_ref[...] = total + acc


def call(kernel, outs, n_in, scratch=(), flops=1_000_000):
    return pl.pallas_call(
        kernel,
        out_shape=[jax.ShapeDtypeStruct(*out) for out in outs],
        in_specs=[pl.BlockSpec(memory_space=pltpu.VMEM)] * n_in,
        out_specs=[pl.BlockSpec(memory_space=pltpu.VMEM)] * len(outs),
        scratch_shapes=list(scratch),
        compiler_params=pltpu.CompilerParams(vmem_limit_bytes=16 * 2**20),
        cost_estimate=pl.CostEstimate(flops=flops, bytes_accessed=2_000_000, transcendentals=0),
    )


def body(
    residual,
    norm_gain,
    w_query,
    w_key,
    w_value,
    w_gate,
    w_input,
    w_forget,
    b_input,
    b_forget,
    w_out,
    memory,
    normalizer,
    stabilizer,
):
    count = lax.axis_size("head")
    batch, width = residual.shape
    rows = w_query.shape[1]
    features = count * width
    (pieces,) = call(spread_kernel, [((count, batch, width), BF16)], 1, flops=SPREAD_FLOPS)(
        residual.astype(BF16)
    )
    gathered = exchange(pieces)

    piece = ((count, batch, width), BF16)
    sources = (
        norm_gain[None],
        w_input,
        w_forget,
        b_input[None],
        b_forget[None],
        normalizer.transpose(1, 2, 0).reshape(H * rows, batch),
        stabilizer.T,
        w_query.reshape(H * rows, features),
        w_key.reshape(H * rows, features),
        w_value,
        w_gate,
        memory,
        repeat_matrix(rows, batch),
    )
    payload, norm_new, stab_new, f_rows, ik_rows, sum_scale, own, floor = call(
        project_kernel,
        [
            ((count, batch + batch // 2 + 4, width), BF16),
            ((H * rows, batch), F32),
            ((H, batch), F32),
            ((H * rows, batch), F32),
            ((H * rows, batch), F32),
            ((batch, width), F32),
            ((batch, width), F32),
            ((batch, width), F32),
        ],
        1 + len(sources),
        scratch=[
            pltpu.VMEM((batch, features), BF16),
            pltpu.VMEM((2, H, 8, width), F32),
            pltpu.VMEM((H, batch), F32),
            pltpu.VMEM((H, batch), F32),
        ],
        flops=100_000_000,
    )(gathered, *sources)
    arrived = exchange(payload)
    (branch,) = call(output_kernel, [piece], 5, flops=30_000_000)(
        arrived, sum_scale, own, floor, w_out
    )
    returned = exchange(branch)
    with jax.named_scope("swap"):
        other = lax.ppermute(arrived[:, batch:], "head", [(i, i ^ 1) for i in range(count)])
    mem_new, norm_out, stab_out = call(
        memory_kernel,
        [(memory.shape, BF16), ((H * rows, batch), F32), ((H, batch), F32)],
        7,
        scratch=[pltpu.VMEM((H, batch, DV), F32)],
        flops=100_000_000,
    )(f_rows, ik_rows, norm_new, stab_new, arrived, other, memory)
    (res_out,) = call(finish_kernel, [((batch, width), F32)], 2)(returned, residual)
    norm_out = norm_out.reshape(H, rows, batch).transpose(2, 0, 1)
    return res_out, mem_new, norm_out, stab_out.T


def solution(mesh):
    in_specs = (
        P("dp", "head"),
        P(),
        P(None, "head", None),
        P(None, "head", None),
        P(None, "head"),
        P(None, "head"),
        P(),
        P(),
        P(),
        P(),
        P("head", None),
        P("dp", None, "head", None),
        P("dp", None, "head"),
        P("dp", None),
    )
    out_specs = (P("dp", "head"), P("dp", None, "head", None), P("dp", None, "head"), P("dp", None))
    return jax.shard_map(body, mesh=mesh, in_specs=in_specs, out_specs=out_specs, check_vma=False)
```

```python
import math

import jax
import jax.numpy as jnp
import numpy as np
from jax import lax
from jax.experimental import pallas as pl
from jax.experimental.pallas import tpu as pltpu
from jax.sharding import PartitionSpec as P

H = 8
DK = 256
DV = 512
EPSILON = 1e-06
F32 = jnp.float32
BF16 = jnp.bfloat16
STATS = 8


SPREAD_FLOPS = 10_000_000_000


def exchange(pieces):
    return lax.all_to_all(pieces, "head", 0, 0, tiled=True)


def dot_last(left, right):
    return lax.dot_general(left, right, (((1,), (1,)), ((), ())), preferred_element_type=F32)


def dot(left, right):
    return jnp.dot(left, right, preferred_element_type=F32)


def column(row):
    n = row.shape[1]
    at_row = lax.broadcasted_iota(jnp.int32, (n, n), 0)
    at_col = lax.broadcasted_iota(jnp.int32, (n, n), 1)
    return jnp.sum(jnp.where(at_row == at_col, row, 0.0), axis=1, keepdims=True)


def split_hi_lo(value):
    high = value.astype(BF16).astype(F32)
    return high, value - high


def repeat_matrix(rows, batch):
    spread = 2 * rows * batch
    col = np.arange(H * spread)
    return jnp.asarray(np.arange(H * rows)[:, None] == col // spread * rows + col % rows, BF16)


def own_mask(rows, batch):
    row = np.arange(4 * batch)[:, None]
    col = np.arange(2 * rows * batch)
    return jnp.asarray((row % batch == col // (2 * rows)) & (row // (2 * batch) == col // rows % 2), BF16)


def spread_kernel(in_ref, out_ref):
    value = in_ref[...]
    for j in range(out_ref.shape[0]):
        out_ref[j] = value


def project_kernel(
    x_ref, gain_ref, wi_ref, wf_ref, bi_ref, bf_ref, nrm_ref, stab_ref, wq_ref, wk_ref, wv_ref, wg_ref, mem_ref,
    repeat_ref, own_ref,
    out_ref, nrm_out_ref, stab_out_ref, f_rows_ref, ik_rows_ref, sum_scale_ref, own_value_ref, floor_ref,
    xn_ref, tail_ref, fg_ref, ig_ref,
):
    pieces, batch, width = x_ref.shape
    half = batch // 2
    rows = wq_ref.shape[0] // H
    total = jnp.zeros((batch, width), F32)
    for j in range(pieces):
        x = x_ref[j].astype(F32)
        total = total + x * x
    mean = jnp.sum(total, axis=1, keepdims=True) / (pieces * width)
    scale = lax.rsqrt(mean + EPSILON)
    tail_ref[...] = jnp.zeros(tail_ref.shape, F32)
    for j in range(pieces):
        cut = slice(j * width, (j + 1) * width)
        xn_ref[:, cut] = (x_ref[j].astype(F32) * scale * gain_ref[:, cut]).astype(BF16)
    x_norm = xn_ref[...]

    left = jnp.concatenate([wq_ref[...], wk_ref[...], wi_ref[...], wf_ref[...]], axis=0)
    mixed = dot_last(left, x_norm)
    query_t = mixed[: H * rows]
    key_t = mixed[H * rows : 2 * H * rows] / math.sqrt(DK)
    input_pre = mixed[2 * H * rows : 2 * H * rows + H] + column(bi_ref[...])
    forget_pre = mixed[2 * H * rows + H :] + column(bf_ref[...])
    log_forget = jnp.minimum(forget_pre, 0.0) - jnp.log1p(jnp.exp(-jnp.abs(forget_pre)))
    kept = log_forget + stab_ref[...]
    stab_new = jnp.maximum(kept, input_pre)
    input_gate = jnp.exp(input_pre - stab_new)
    forget_gate = jnp.exp(kept - stab_new)
    stab_out_ref[...] = stab_new
    fg_ref[...] = forget_gate
    ig_ref[...] = input_gate

    for h in range(H):
        part = slice(h * rows, (h + 1) * rows)
        key_h = key_t[part]
        query_h = query_t[part]
        f_h = jnp.broadcast_to(forget_gate[h : h + 1], (rows, batch))
        ik_h = input_gate[h : h + 1] * key_h
        norm_h = f_h * nrm_ref[part] + ik_h
        nrm_out_ref[part] = norm_h
        f_rows_ref[part] = f_h
        ik_rows_ref[part] = ik_h
        norm_query = jnp.sum(norm_h * query_h, axis=0, keepdims=True)
        key_query = jnp.sum(key_h * query_h, axis=0, keepdims=True)
        kinds = (*split_hi_lo(norm_query), *split_hi_lo(key_query))
        for k, kind in enumerate(kinds):
            for core in range(2):
                tail_ref[core, h, 4 + k : 5 + k, :batch] = kind

    spread = batch * rows
    high, low = split_hi_lo(query_t.T)
    both = jnp.concatenate([high, low], axis=0).astype(BF16)
    spread = repeat_ref.shape[1] // H
    wide = dot(both, repeat_ref[...]).astype(BF16)
    share = pieces // H
    deep = 2 * rows
    for h in range(H):
        wide_h = wide[:, h * spread : (h + 1) * spread]
        left = jnp.concatenate([wide_h, wide_h], axis=0) * own_ref[...]
        right = [mem_ref[:, h, k * deep : (k + 1) * deep].reshape(spread, width) for k in range(2)]
        product = dot(left, jnp.concatenate(right, axis=1))
        for parity in range(2):
            at = parity * 2 * batch
            numer = (product[at : at + batch] + product[at + batch : at + 2 * batch]).astype(BF16)
            for k in range(2):
                out_ref[h * share + 2 * k + parity, :batch] = numer[:, k * width : (k + 1) * width]

    value_gate = dot(x_norm, jnp.concatenate([wv_ref[...], wg_ref[...]], axis=1))
    value = value_gate[:, :width]
    for core in range(2):
        first = value[core * half : core * half + 8].astype(BF16)
        rest = value[core * half + 8 : (core + 1) * half]
        for h in range(H):
            tail_ref[core, h, :4] = rest
        for j in range(core, pieces, 2):
            out_ref[j, batch : batch + 8] = first
            out_ref[j, batch + 8 :] = tail_ref[core, j // share].astype(BF16)

    head = lax.axis_index("head") * width // DV
    pick = lambda ref: column(ref[pl.ds(head, 1), :])
    gate = jax.nn.sigmoid(value_gate[:, width:])
    sum_scale_ref[...] = gate * pick(fg_ref)
    own_value_ref[...] = gate * (pick(ig_ref) * value.astype(BF16).astype(F32))
    floor_ref[...] = jnp.broadcast_to(jnp.exp(-pick(stab_out_ref)), floor_ref.shape)


def output_kernel(in_ref, sum_scale_ref, own_ref, floor_ref, wo_ref, out_ref):
    pieces, batch, width = out_ref.shape
    total = in_ref[0, :batch].astype(F32)
    tail = in_ref[0, batch + 8 :].astype(F32)
    for j in range(1, pieces):
        total = total + in_ref[j, :batch].astype(F32)
        tail = tail + in_ref[j, batch + 8 :].astype(F32)
    norm_query = column(tail[4:5, :batch] + tail[5:6, :batch])
    key_query = column(tail[6:7, :batch] + tail[7:8, :batch])
    numer = sum_scale_ref[...] * total + own_ref[...] * key_query
    hidden = (numer / jnp.maximum(jnp.abs(norm_query), floor_ref[...])).astype(BF16)
    for j in range(0, pieces, 2):
        pair = dot(hidden, wo_ref[:, j * width : (j + 2) * width]).astype(BF16)
        out_ref[j] = pair[:, :width]
        out_ref[j + 1] = pair[:, width:]


def memory_kernel(
    f_rows_ref, ik_rows_ref, norm_ref, stab_ref, mine_ref, other_ref, mem_ref,
    out_ref, norm_out_ref, stab_out_ref, wide_ref,
):
    norm_out_ref[...] = norm_ref[...]
    stab_out_ref[...] = stab_ref[...]
    pieces = mine_ref.shape[0]
    batch, _, rows, _ = mem_ref.shape
    width = mine_ref.shape[2]
    half = batch // 2
    share = pieces // H
    even = lax.axis_index("head") % 2 == 0
    for j in range(pieces):
        cut = slice((j % share) * width, (j % share + 1) * width)
        mine = mine_ref[j, batch : batch + 16].astype(F32)[:half]
        other = other_ref[j].astype(F32)[:half]
        wide_ref[j // share, :half, cut] = jnp.where(even, mine, other)
        wide_ref[j // share, half:, cut] = jnp.where(even, other, mine)

    def one_head(h, carry):
        at = pl.multiple_of(h * rows, rows)
        f_rows = f_rows_ref[pl.ds(at, rows), :]
        ik_rows = ik_rows_ref[pl.ds(at, rows), :]
        for b in range(batch):
            kept = f_rows[:, b : b + 1] * mem_ref[b, h].astype(F32)
            out_ref[b, h] = (kept + ik_rows[:, b : b + 1] * wide_ref[h, b : b + 1, :]).astype(BF16)
        return carry

    lax.fori_loop(0, H, one_head, 0)


def finish_kernel(in_ref, residual_ref, out_ref):
    total = residual_ref[...]
    acc = in_ref[0].astype(F32)
    for j in range(1, in_ref.shape[0]):
        acc = acc + in_ref[j].astype(F32)
    out_ref[...] = total + acc


def call(kernel, outs, n_in, scratch=(), flops=1_000_000):
    return pl.pallas_call(
        kernel,
        out_shape=[jax.ShapeDtypeStruct(*out) for out in outs],
        in_specs=[pl.BlockSpec(memory_space=pltpu.VMEM)] * n_in,
        out_specs=[pl.BlockSpec(memory_space=pltpu.VMEM)] * len(outs),
        scratch_shapes=list(scratch),
        compiler_params=pltpu.CompilerParams(vmem_limit_bytes=16 * 2**20),
        cost_estimate=pl.CostEstimate(flops=flops, bytes_accessed=2_000_000, transcendentals=0),
    )


def body(
    residual,
    norm_gain,
    w_query,
    w_key,
    w_value,
    w_gate,
    w_input,
    w_forget,
    b_input,
    b_forget,
    w_out,
    memory,
    normalizer,
    stabilizer,
):
    count = lax.axis_size("head")
    batch, width = residual.shape
    rows = w_query.shape[1]
    features = count * width
    (pieces,) = call(spread_kernel, [((count, batch, width), BF16)], 1, flops=SPREAD_FLOPS)(
        residual.astype(BF16)
    )
    gathered = exchange(pieces)

    piece = ((count, batch, width), BF16)
    sources = (
        norm_gain[None],
        w_input,
        w_forget,
        b_input[None],
        b_forget[None],
        normalizer.transpose(1, 2, 0).reshape(H * rows, batch),
        stabilizer.T,
        w_query.reshape(H * rows, features),
        w_key.reshape(H * rows, features),
        w_value,
        w_gate,
        memory.reshape(batch, H, rows, DV // width, width)
        .transpose(0, 1, 3, 2, 4)
        .reshape(batch, H, DV // width * rows, width),
        repeat_matrix(rows, batch),
        own_mask(rows, batch),
    )
    payload, norm_new, stab_new, f_rows, ik_rows, sum_scale, own, floor = call(
        project_kernel,
        [
            ((count, batch + batch // 2 + 4, width), BF16),
            ((H * rows, batch), F32),
            ((H, batch), F32),
            ((H * rows, batch), F32),
            ((H * rows, batch), F32),
            ((batch, width), F32),
            ((batch, width), F32),
            ((batch, width), F32),
        ],
        1 + len(sources),
        scratch=[
            pltpu.VMEM((batch, features), BF16),
            pltpu.VMEM((2, H, 8, width), F32),
            pltpu.VMEM((H, batch), F32),
            pltpu.VMEM((H, batch), F32),
        ],
        flops=100_000_000,
    )(gathered, *sources)
    arrived = exchange(payload)
    (branch,) = call(output_kernel, [piece], 5, flops=30_000_000)(
        arrived, sum_scale, own, floor, w_out
    )
    returned = exchange(branch)
    with jax.named_scope("swap"):
        other = lax.ppermute(arrived[:, batch:], "head", [(i, i ^ 1) for i in range(count)])
    mem_new, norm_out, stab_out = call(
        memory_kernel,
        [(memory.shape, BF16), ((H * rows, batch), F32), ((H, batch), F32)],
        7,
        scratch=[pltpu.VMEM((H, batch, DV), F32)],
        flops=100_000_000,
    )(f_rows, ik_rows, norm_new, stab_new, arrived, other, memory)
    (res_out,) = call(finish_kernel, [((batch, width), F32)], 2)(returned, residual)
    norm_out = norm_out.reshape(H, rows, batch).transpose(2, 0, 1)
    return res_out, mem_new, norm_out, stab_out.T


def solution(mesh):
    in_specs = (
        P("dp", "head"),
        P(),
        P(None, "head", None),
        P(None, "head", None),
        P(None, "head"),
        P(None, "head"),
        P(),
        P(),
        P(),
        P(),
        P("head", None),
        P("dp", None, "head", None),
        P("dp", None, "head"),
        P("dp", None),
    )
    out_specs = (P("dp", "head"), P("dp", None, "head", None), P("dp", None, "head"), P("dp", None))
    return jax.shard_map(body, mesh=mesh, in_specs=in_specs, out_specs=out_specs, check_vma=False)
```

```python
import math

import jax
import jax.numpy as jnp
import numpy as np
from jax import lax
from jax.experimental import pallas as pl
from jax.experimental.pallas import tpu as pltpu
from jax.sharding import PartitionSpec as P

H = 8
DK = 256
DV = 512
EPSILON = 1e-06
F32 = jnp.float32
BF16 = jnp.bfloat16
STATS = 8


FAR = 21
SPREAD_FLOPS = 10_000_000_000


def exchange(pieces, far=0):
    count = lax.axis_size("head")
    return lax.all_to_all(
        pieces, "head", 0, 0, tiled=True, axis_index_groups=[[k ^ far for k in range(count)]]
    )


def dot_last(left, right):
    return lax.dot_general(left, right, (((1,), (1,)), ((), ())), preferred_element_type=F32)


def dot(left, right):
    return jnp.dot(left, right, preferred_element_type=F32)


def column(row):
    n = row.shape[1]
    at_row = lax.broadcasted_iota(jnp.int32, (n, n), 0)
    at_col = lax.broadcasted_iota(jnp.int32, (n, n), 1)
    return jnp.sum(jnp.where(at_row == at_col, row, 0.0), axis=1, keepdims=True)


def split_hi_lo(value):
    high = value.astype(BF16).astype(F32)
    return high, value - high


def repeat_matrix(rows, batch):
    spread = 2 * rows * batch
    col = np.arange(H * spread)
    return jnp.asarray(np.arange(H * rows)[:, None] == col // spread * rows + col % rows, BF16)


def own_mask(rows, batch):
    row = np.arange(4 * batch)[:, None]
    col = np.arange(2 * rows * batch)
    return jnp.asarray((row % batch == col // (2 * rows)) & (row // (2 * batch) == col // rows % 2), BF16)


def spread_kernel(in_ref, out_ref):
    value = in_ref[...]
    for j in range(out_ref.shape[0]):
        out_ref[j] = value


def project_kernel(
    x_ref, gain_ref, wi_ref, wf_ref, bi_ref, bf_ref, nrm_ref, stab_ref, wq_ref, wk_ref, wv_ref, wg_ref, mem_ref,
    repeat_ref, own_ref,
    out_ref, nrm_out_ref, stab_out_ref, f_rows_ref, ik_rows_ref, sum_scale_ref, own_value_ref, floor_ref,
    xn_ref, tail_ref, fg_ref, ig_ref,
):
    pieces, batch, width = x_ref.shape
    half = batch // 2
    rows = wq_ref.shape[0] // H
    total = jnp.zeros((batch, width), F32)
    for j in range(pieces):
        x = x_ref[j].astype(F32)
        total = total + x * x
    mean = jnp.sum(total, axis=1, keepdims=True) / (pieces * width)
    scale = lax.rsqrt(mean + EPSILON)
    tail_ref[...] = jnp.zeros(tail_ref.shape, F32)
    for j in range(pieces):
        cut = slice((j ^ FAR) * width, ((j ^ FAR) + 1) * width)
        xn_ref[:, cut] = (x_ref[j].astype(F32) * scale * gain_ref[:, cut]).astype(BF16)
    x_norm = xn_ref[...]

    left = jnp.concatenate([wq_ref[...], wk_ref[...], wi_ref[...], wf_ref[...]], axis=0)
    mixed = dot_last(left, x_norm)
    query_t = mixed[: H * rows]
    key_t = mixed[H * rows : 2 * H * rows] / math.sqrt(DK)
    input_pre = mixed[2 * H * rows : 2 * H * rows + H] + column(bi_ref[...])
    forget_pre = mixed[2 * H * rows + H :] + column(bf_ref[...])
    log_forget = jnp.minimum(forget_pre, 0.0) - jnp.log1p(jnp.exp(-jnp.abs(forget_pre)))
    kept = log_forget + stab_ref[...]
    stab_new = jnp.maximum(kept, input_pre)
    input_gate = jnp.exp(input_pre - stab_new)
    forget_gate = jnp.exp(kept - stab_new)
    stab_out_ref[...] = stab_new
    fg_ref[...] = forget_gate
    ig_ref[...] = input_gate

    for h in range(H):
        part = slice(h * rows, (h + 1) * rows)
        key_h = key_t[part]
        query_h = query_t[part]
        f_h = jnp.broadcast_to(forget_gate[h : h + 1], (rows, batch))
        ik_h = input_gate[h : h + 1] * key_h
        norm_h = f_h * nrm_ref[part] + ik_h
        nrm_out_ref[part] = norm_h
        f_rows_ref[part] = f_h
        ik_rows_ref[part] = ik_h
        norm_query = jnp.sum(norm_h * query_h, axis=0, keepdims=True)
        key_query = jnp.sum(key_h * query_h, axis=0, keepdims=True)
        kinds = (*split_hi_lo(norm_query), *split_hi_lo(key_query))
        for k, kind in enumerate(kinds):
            for core in range(2):
                tail_ref[core, h, 4 + k : 5 + k, :batch] = kind

    spread = batch * rows
    high, low = split_hi_lo(query_t.T)
    both = jnp.concatenate([high, low], axis=0).astype(BF16)
    spread = repeat_ref.shape[1] // H
    wide = dot(both, repeat_ref[...]).astype(BF16)
    share = pieces // H
    deep = 2 * rows
    for h in range(H):
        wide_h = wide[:, h * spread : (h + 1) * spread]
        left = jnp.concatenate([wide_h, wide_h], axis=0) * own_ref[...]
        right = [mem_ref[:, h, k * deep : (k + 1) * deep].reshape(spread, width) for k in range(2)]
        product = dot(left, jnp.concatenate(right, axis=1))
        for parity in range(2):
            at = parity * 2 * batch
            numer = (product[at : at + batch] + product[at + batch : at + 2 * batch]).astype(BF16)
            for k in range(2):
                out_ref[(h * share + 2 * k + parity) ^ FAR, :batch] = numer[:, k * width : (k + 1) * width]

    value_gate = dot(x_norm, jnp.concatenate([wv_ref[...], wg_ref[...]], axis=1))
    value = value_gate[:, :width]
    for core in range(2):
        first = value[core * half : core * half + 8].astype(BF16)
        rest = value[core * half + 8 : (core + 1) * half]
        for h in range(H):
            tail_ref[core, h, :4] = rest
        for j in range(core, pieces, 2):
            out_ref[j ^ FAR, batch : batch + 8] = first
            out_ref[j ^ FAR, batch + 8 :] = tail_ref[core, j // share].astype(BF16)

    head = lax.axis_index("head") * width // DV
    pick = lambda ref: column(ref[pl.ds(head, 1), :])
    gate = jax.nn.sigmoid(value_gate[:, width:])
    sum_scale_ref[...] = gate * pick(fg_ref)
    own_value_ref[...] = gate * (pick(ig_ref) * value.astype(BF16).astype(F32))
    floor_ref[...] = jnp.broadcast_to(jnp.exp(-pick(stab_out_ref)), floor_ref.shape)


def output_kernel(in_ref, sum_scale_ref, own_ref, floor_ref, wo_ref, out_ref):
    pieces, batch, width = out_ref.shape
    total = in_ref[0, :batch].astype(F32)
    tail = in_ref[0, batch + 8 :].astype(F32)
    for j in range(1, pieces):
        total = total + in_ref[j, :batch].astype(F32)
        tail = tail + in_ref[j, batch + 8 :].astype(F32)
    norm_query = column(tail[4:5, :batch] + tail[5:6, :batch])
    key_query = column(tail[6:7, :batch] + tail[7:8, :batch])
    numer = sum_scale_ref[...] * total + own_ref[...] * key_query
    hidden = (numer / jnp.maximum(jnp.abs(norm_query), floor_ref[...])).astype(BF16)
    for j in range(0, pieces, 2):
        pair = dot(hidden, wo_ref[:, j * width : (j + 2) * width]).astype(BF16)
        out_ref[j ^ FAR] = pair[:, :width]
        out_ref[(j + 1) ^ FAR] = pair[:, width:]


def memory_kernel(
    f_rows_ref, ik_rows_ref, norm_ref, stab_ref, mine_ref, other_ref, mem_ref,
    out_ref, norm_out_ref, stab_out_ref, wide_ref,
):
    norm_out_ref[...] = norm_ref[...]
    stab_out_ref[...] = stab_ref[...]
    pieces = mine_ref.shape[0]
    batch, _, rows, _ = mem_ref.shape
    width = mine_ref.shape[2]
    half = batch // 2
    share = pieces // H
    even = lax.axis_index("head") % 2 == 0
    for j in range(pieces):
        cut = slice((j % share) * width, (j % share + 1) * width)
        mine = mine_ref[j ^ FAR, batch : batch + 16].astype(F32)[:half]
        other = other_ref[j ^ FAR].astype(F32)[:half]
        wide_ref[j // share, :half, cut] = jnp.where(even, mine, other)
        wide_ref[j // share, half:, cut] = jnp.where(even, other, mine)

    def one_head(h, carry):
        at = pl.multiple_of(h * rows, rows)
        f_rows = f_rows_ref[pl.ds(at, rows), :]
        ik_rows = ik_rows_ref[pl.ds(at, rows), :]
        for b in range(batch):
            kept = f_rows[:, b : b + 1] * mem_ref[b, h].astype(F32)
            out_ref[b, h] = (kept + ik_rows[:, b : b + 1] * wide_ref[h, b : b + 1, :]).astype(BF16)
        return carry

    lax.fori_loop(0, H, one_head, 0)


def finish_kernel(in_ref, residual_ref, out_ref):
    total = residual_ref[...]
    acc = in_ref[0].astype(F32)
    for j in range(1, in_ref.shape[0]):
        acc = acc + in_ref[j].astype(F32)
    out_ref[...] = total + acc


def call(kernel, outs, n_in, scratch=(), flops=1_000_000):
    return pl.pallas_call(
        kernel,
        out_shape=[jax.ShapeDtypeStruct(*out) for out in outs],
        in_specs=[pl.BlockSpec(memory_space=pltpu.VMEM)] * n_in,
        out_specs=[pl.BlockSpec(memory_space=pltpu.VMEM)] * len(outs),
        scratch_shapes=list(scratch),
        compiler_params=pltpu.CompilerParams(vmem_limit_bytes=16 * 2**20),
        cost_estimate=pl.CostEstimate(flops=flops, bytes_accessed=2_000_000, transcendentals=0),
    )


def body(
    residual,
    norm_gain,
    w_query,
    w_key,
    w_value,
    w_gate,
    w_input,
    w_forget,
    b_input,
    b_forget,
    w_out,
    memory,
    normalizer,
    stabilizer,
):
    count = lax.axis_size("head")
    batch, width = residual.shape
    rows = w_query.shape[1]
    features = count * width
    (pieces,) = call(spread_kernel, [((count, batch, width), BF16)], 1, flops=SPREAD_FLOPS)(
        residual.astype(BF16)
    )
    gathered = exchange(pieces, FAR)

    piece = ((count, batch, width), BF16)
    sources = (
        norm_gain[None],
        w_input,
        w_forget,
        b_input[None],
        b_forget[None],
        normalizer.transpose(1, 2, 0).reshape(H * rows, batch),
        stabilizer.T,
        w_query.reshape(H * rows, features),
        w_key.reshape(H * rows, features),
        w_value,
        w_gate,
        memory.reshape(batch, H, rows, DV // width, width)
        .transpose(0, 1, 3, 2, 4)
        .reshape(batch, H, DV // width * rows, width),
        repeat_matrix(rows, batch),
        own_mask(rows, batch),
    )
    payload, norm_new, stab_new, f_rows, ik_rows, sum_scale, own, floor = call(
        project_kernel,
        [
            ((count, batch + batch // 2 + 4, width), BF16),
            ((H * rows, batch), F32),
            ((H, batch), F32),
            ((H * rows, batch), F32),
            ((H * rows, batch), F32),
            ((batch, width), F32),
            ((batch, width), F32),
            ((batch, width), F32),
        ],
        1 + len(sources),
        scratch=[
            pltpu.VMEM((batch, features), BF16),
            pltpu.VMEM((2, H, 8, width), F32),
            pltpu.VMEM((H, batch), F32),
            pltpu.VMEM((H, batch), F32),
        ],
        flops=100_000_000,
    )(gathered, *sources)
    arrived = exchange(payload, FAR)
    (branch,) = call(output_kernel, [piece], 5, flops=30_000_000)(
        arrived, sum_scale, own, floor, w_out
    )
    returned = exchange(branch, FAR)
    with jax.named_scope("swap"):
        other = lax.ppermute(arrived[:, batch:], "head", [(i, i ^ 1) for i in range(count)])
    mem_new, norm_out, stab_out = call(
        memory_kernel,
        [(memory.shape, BF16), ((H * rows, batch), F32), ((H, batch), F32)],
        7,
        scratch=[pltpu.VMEM((H, batch, DV), F32)],
        flops=100_000_000,
    )(f_rows, ik_rows, norm_new, stab_new, arrived, other, memory)
    (res_out,) = call(finish_kernel, [((batch, width), F32)], 2)(returned, residual)
    norm_out = norm_out.reshape(H, rows, batch).transpose(2, 0, 1)
    return res_out, mem_new, norm_out, stab_out.T


def solution(mesh):
    in_specs = (
        P("dp", "head"),
        P(),
        P(None, "head", None),
        P(None, "head", None),
        P(None, "head"),
        P(None, "head"),
        P(),
        P(),
        P(),
        P(),
        P("head", None),
        P("dp", None, "head", None),
        P("dp", None, "head"),
        P("dp", None),
    )
    out_specs = (P("dp", "head"), P("dp", None, "head", None), P("dp", None, "head"), P("dp", None))
    return jax.shard_map(body, mesh=mesh, in_specs=in_specs, out_specs=out_specs, check_vma=False)
```

```python
import math

import jax
import jax.numpy as jnp
import numpy as np
from jax import lax
from jax.experimental import pallas as pl
from jax.experimental.pallas import tpu as pltpu
from jax.sharding import PartitionSpec as P

H = 8
DK = 256
DV = 512
EPSILON = 1e-06
F32 = jnp.float32
BF16 = jnp.bfloat16
STATS = 8


CHUNKS = 3
FAR = 21
SPREAD_FLOPS = 10_000_000_000


def exchange(pieces, far=0):
    count = lax.axis_size("head")
    return lax.all_to_all(
        pieces, "head", 0, 0, tiled=True, axis_index_groups=[[k ^ far for k in range(count)]]
    )


def dot_last(left, right):
    return lax.dot_general(left, right, (((1,), (1,)), ((), ())), preferred_element_type=F32)


def dot(left, right):
    return jnp.dot(left, right, preferred_element_type=F32)


def column(row):
    n = row.shape[1]
    at_row = lax.broadcasted_iota(jnp.int32, (n, n), 0)
    at_col = lax.broadcasted_iota(jnp.int32, (n, n), 1)
    return jnp.sum(jnp.where(at_row == at_col, row, 0.0), axis=1, keepdims=True)


def split_hi_lo(value):
    high = value.astype(BF16).astype(F32)
    return high, value - high


def repeat_matrix(rows, batch):
    spread = 2 * rows * batch
    col = np.arange(H * spread)
    return jnp.asarray(np.arange(H * rows)[:, None] == col // spread * rows + col % rows, BF16)


def own_mask(rows, batch):
    row = np.arange(4 * batch)[:, None]
    col = np.arange(2 * rows * batch)
    return jnp.asarray((row % batch == col // (2 * rows)) & (row // (2 * batch) == col // rows % 2), BF16)


def spread_kernel(in_ref, out_ref):
    value = in_ref[...]
    for j in range(out_ref.shape[0]):
        out_ref[j] = value


def project_kernel(
    x_ref, gain_ref, wi_ref, wf_ref, bi_ref, bf_ref, nrm_ref, stab_ref, wq_ref, wk_ref, wv_ref, wg_ref, mem_ref,
    repeat_ref, own_ref,
    out_ref, nrm_out_ref, stab_out_ref, f_rows_ref, ik_rows_ref, sum_scale_ref, own_value_ref, floor_ref,
    xn_ref, tail_ref, fg_ref, ig_ref,
):
    pieces, batch, width = x_ref.shape
    half = batch // 2
    rows = wq_ref.shape[0] // H
    total = jnp.zeros((batch, width), F32)
    for j in range(pieces):
        x = x_ref[j].astype(F32)
        total = total + x * x
    mean = jnp.sum(total, axis=1, keepdims=True) / (pieces * width)
    scale = lax.rsqrt(mean + EPSILON)
    tail_ref[...] = jnp.zeros(tail_ref.shape, F32)
    for j in range(pieces):
        cut = slice((j ^ FAR) * width, ((j ^ FAR) + 1) * width)
        xn_ref[:, cut] = (x_ref[j].astype(F32) * scale * gain_ref[:, cut]).astype(BF16)
    x_norm = xn_ref[...]

    left = jnp.concatenate([wq_ref[...], wk_ref[...], wi_ref[...], wf_ref[...]], axis=0)
    mixed = dot_last(left, x_norm)
    query_t = mixed[: H * rows]
    key_t = mixed[H * rows : 2 * H * rows] / math.sqrt(DK)
    input_pre = mixed[2 * H * rows : 2 * H * rows + H] + column(bi_ref[...])
    forget_pre = mixed[2 * H * rows + H :] + column(bf_ref[...])
    log_forget = jnp.minimum(forget_pre, 0.0) - jnp.log1p(jnp.exp(-jnp.abs(forget_pre)))
    kept = log_forget + stab_ref[...]
    stab_new = jnp.maximum(kept, input_pre)
    input_gate = jnp.exp(input_pre - stab_new)
    forget_gate = jnp.exp(kept - stab_new)
    stab_out_ref[...] = stab_new
    fg_ref[...] = forget_gate
    ig_ref[...] = input_gate

    for h in range(H):
        part = slice(h * rows, (h + 1) * rows)
        key_h = key_t[part]
        query_h = query_t[part]
        f_h = jnp.broadcast_to(forget_gate[h : h + 1], (rows, batch))
        ik_h = input_gate[h : h + 1] * key_h
        norm_h = f_h * nrm_ref[part] + ik_h
        nrm_out_ref[part] = norm_h
        f_rows_ref[part] = f_h
        ik_rows_ref[part] = ik_h
        norm_query = jnp.sum(norm_h * query_h, axis=0, keepdims=True)
        key_query = jnp.sum(key_h * query_h, axis=0, keepdims=True)
        kinds = (*split_hi_lo(norm_query), *split_hi_lo(key_query))
        for k, kind in enumerate(kinds):
            for core in range(2):
                tail_ref[core, h, 4 + k : 5 + k, :batch] = kind

    spread = batch * rows
    high, low = split_hi_lo(query_t.T)
    both = jnp.concatenate([high, low], axis=0).astype(BF16)
    spread = repeat_ref.shape[1] // H
    wide = dot(both, repeat_ref[...]).astype(BF16)
    share = pieces // H
    deep = 2 * rows
    for h in range(H):
        wide_h = wide[:, h * spread : (h + 1) * spread]
        left = jnp.concatenate([wide_h, wide_h], axis=0) * own_ref[...]
        right = [mem_ref[:, h, k * deep : (k + 1) * deep].reshape(spread, width) for k in range(2)]
        product = dot(left, jnp.concatenate(right, axis=1))
        for parity in range(2):
            at = parity * 2 * batch
            numer = (product[at : at + batch] + product[at + batch : at + 2 * batch]).astype(BF16)
            for k in range(2):
                out_ref[(h * share + 2 * k + parity) ^ FAR, :batch] = numer[:, k * width : (k + 1) * width]

    value_gate = dot(x_norm, jnp.concatenate([wv_ref[...], wg_ref[...]], axis=1))
    value = value_gate[:, :width]
    for core in range(2):
        first = value[core * half : core * half + 8].astype(BF16)
        rest = value[core * half + 8 : (core + 1) * half]
        for h in range(H):
            tail_ref[core, h, :4] = rest
        for j in range(core, pieces, 2):
            out_ref[j ^ FAR, batch : batch + 8] = first
            out_ref[j ^ FAR, batch + 8 :] = tail_ref[core, j // share].astype(BF16)

    head = lax.axis_index("head") * width // DV
    pick = lambda ref: column(ref[pl.ds(head, 1), :])
    gate = jax.nn.sigmoid(value_gate[:, width:])
    sum_scale_ref[...] = gate * pick(fg_ref)
    own_value_ref[...] = gate * (pick(ig_ref) * value.astype(BF16).astype(F32))
    floor_ref[...] = jnp.broadcast_to(jnp.exp(-pick(stab_out_ref)), floor_ref.shape)


def output_kernel(in_ref, sum_scale_ref, own_ref, floor_ref, wo_ref, out_ref):
    pieces, batch, width = out_ref.shape
    total = in_ref[0, :batch].astype(F32)
    tail = in_ref[0, batch + 8 :].astype(F32)
    for j in range(1, pieces):
        total = total + in_ref[j, :batch].astype(F32)
        tail = tail + in_ref[j, batch + 8 :].astype(F32)
    norm_query = column(tail[4:5, :batch] + tail[5:6, :batch])
    key_query = column(tail[6:7, :batch] + tail[7:8, :batch])
    numer = sum_scale_ref[...] * total + own_ref[...] * key_query
    hidden = (numer / jnp.maximum(jnp.abs(norm_query), floor_ref[...])).astype(BF16)
    for j in range(0, pieces, 2):
        pair = dot(hidden, wo_ref[:, j * width : (j + 2) * width]).astype(BF16)
        out_ref[j ^ FAR] = pair[:, :width]
        out_ref[(j + 1) ^ FAR] = pair[:, width:]


def memory_half(side, f_rows_ref, ik_rows_ref, half_ref, mem_ref, out_hbm, wide_ref, new_ref, sems):
    pieces, depth, width = half_ref.shape
    _, _, rows, _ = mem_ref.shape
    half = wide_ref.shape[1]
    share = pieces // H
    first = depth - 16
    lower = lax.axis_index("head") % 2 == side
    base = jnp.where(lower, 0, half)
    for j in range(pieces):
        cut = slice((j % share) * width, (j % share + 1) * width)
        wide_ref[j // share, :, cut] = half_ref[j ^ FAR, first:].astype(F32)[:half]

    f_mine = jnp.where(lower, f_rows_ref[:, :half], f_rows_ref[:, half:])
    ik_mine = jnp.where(lower, ik_rows_ref[:, :half], ik_rows_ref[:, half:])
    step = half // CHUNKS
    copies = []
    for k in range(CHUNKS):
        for h in range(H):
            part = slice(h * rows, (h + 1) * rows)
            for i in range(k * step, (k + 1) * step):
                kept = f_mine[part, i : i + 1] * mem_ref[base + i, h].astype(F32)
                added = ik_mine[part, i : i + 1] * wide_ref[h, i : i + 1, :]
                new_ref[i, h] = (kept + added).astype(BF16)
        source = new_ref.at[k * step : (k + 1) * step]
        target = out_hbm.at[pl.ds(base + k * step, step)]
        copies.append(pltpu.make_async_copy(source, target, sems.at[k]))
        copies[-1].start()
    for copy in copies:
        copy.wait()


def memory_mine_kernel(
    f_rows_ref, ik_rows_ref, norm_ref, stab_ref, half_ref, mem_ref,
    out_hbm, norm_out_hbm, stab_out_hbm, wide_ref, new_ref, sems, small_sems,
):
    norm_copy = pltpu.make_async_copy(norm_ref, norm_out_hbm, small_sems.at[0])
    stab_copy = pltpu.make_async_copy(stab_ref, stab_out_hbm, small_sems.at[1])
    norm_copy.start()
    stab_copy.start()
    memory_half(0, f_rows_ref, ik_rows_ref, half_ref, mem_ref, out_hbm, wide_ref, new_ref, sems)
    norm_copy.wait()
    stab_copy.wait()


def memory_other_kernel(
    f_rows_ref, ik_rows_ref, half_ref, mem_ref, partial_hbm, out_hbm, wide_ref, new_ref, sems
):
    del partial_hbm
    memory_half(1, f_rows_ref, ik_rows_ref, half_ref, mem_ref, out_hbm, wide_ref, new_ref, sems)


def finish_kernel(in_ref, residual_ref, out_ref):
    total = residual_ref[...]
    acc = in_ref[0].astype(F32)
    for j in range(1, in_ref.shape[0]):
        acc = acc + in_ref[j].astype(F32)
    out_ref[...] = total + acc


def call(kernel, outs, n_in, scratch=(), flops=1_000_000, hbm_out=False, alias=False):
    vmem, hbm = (pl.BlockSpec(memory_space=space) for space in (pltpu.VMEM, pltpu.HBM))
    return pl.pallas_call(
        kernel,
        out_shape=[jax.ShapeDtypeStruct(*out) for out in outs],
        in_specs=[vmem] * n_in + [hbm] * alias,
        out_specs=[hbm if hbm_out else vmem] * len(outs),
        scratch_shapes=list(scratch),
        input_output_aliases={n_in: 0} if alias else {},
        compiler_params=pltpu.CompilerParams(vmem_limit_bytes=16 * 2**20),
        cost_estimate=pl.CostEstimate(flops=flops, bytes_accessed=2_000_000, transcendentals=0),
    )


def body(
    residual,
    norm_gain,
    w_query,
    w_key,
    w_value,
    w_gate,
    w_input,
    w_forget,
    b_input,
    b_forget,
    w_out,
    memory,
    normalizer,
    stabilizer,
):
    count = lax.axis_size("head")
    batch, width = residual.shape
    rows = w_query.shape[1]
    features = count * width
    (pieces,) = call(spread_kernel, [((count, batch, width), BF16)], 1, flops=SPREAD_FLOPS)(
        residual.astype(BF16)
    )
    gathered = exchange(pieces, FAR)

    piece = ((count, batch, width), BF16)
    sources = (
        norm_gain[None],
        w_input,
        w_forget,
        b_input[None],
        b_forget[None],
        normalizer.transpose(1, 2, 0).reshape(H * rows, batch),
        stabilizer.T,
        w_query.reshape(H * rows, features),
        w_key.reshape(H * rows, features),
        w_value,
        w_gate,
        memory.reshape(batch, H, rows, DV // width, width)
        .transpose(0, 1, 3, 2, 4)
        .reshape(batch, H, DV // width * rows, width),
        repeat_matrix(rows, batch),
        own_mask(rows, batch),
    )
    payload, norm_new, stab_new, f_rows, ik_rows, sum_scale, own, floor = call(
        project_kernel,
        [
            ((count, batch + batch // 2 + 4, width), BF16),
            ((H * rows, batch), F32),
            ((H, batch), F32),
            ((H * rows, batch), F32),
            ((H * rows, batch), F32),
            ((batch, width), F32),
            ((batch, width), F32),
            ((batch, width), F32),
        ],
        1 + len(sources),
        scratch=[
            pltpu.VMEM((batch, features), BF16),
            pltpu.VMEM((2, H, 8, width), F32),
            pltpu.VMEM((H, batch), F32),
            pltpu.VMEM((H, batch), F32),
        ],
        flops=100_000_000,
    )(gathered, *sources)
    arrived = exchange(payload, FAR)
    (branch,) = call(output_kernel, [piece], 5, flops=30_000_000)(
        arrived, sum_scale, own, floor, w_out
    )
    returned = exchange(branch, FAR)
    with jax.named_scope("swap"):
        other = lax.ppermute(arrived[:, batch:], "head", [(i, i ^ 1) for i in range(count)])
    half_scratch = [
        pltpu.VMEM((H, batch // 2, DV), F32),
        pltpu.VMEM((batch // 2, *memory.shape[1:]), BF16),
        pltpu.SemaphoreType.DMA((CHUNKS,)),
    ]
    mem_half, norm_out, stab_out = call(
        memory_mine_kernel,
        [(memory.shape, BF16), ((H * rows, batch), F32), ((H, batch), F32)],
        6,
        scratch=[*half_scratch, pltpu.SemaphoreType.DMA((2,))],
        flops=50_000_000,
        hbm_out=True,
    )(f_rows, ik_rows, norm_new, stab_new, arrived, memory)
    (mem_new,) = call(
        memory_other_kernel,
        [(memory.shape, BF16)],
        4,
        scratch=half_scratch,
        flops=50_000_000,
        hbm_out=True,
        alias=True,
    )(f_rows, ik_rows, other, memory, mem_half)
    (res_out,) = call(finish_kernel, [((batch, width), F32)], 2)(returned, residual)
    norm_out = norm_out.reshape(H, rows, batch).transpose(2, 0, 1)
    return res_out, mem_new, norm_out, stab_out.T


def solution(mesh):
    in_specs = (
        P("dp", "head"),
        P(),
        P(None, "head", None),
        P(None, "head", None),
        P(None, "head"),
        P(None, "head"),
        P(),
        P(),
        P(),
        P(),
        P("head", None),
        P("dp", None, "head", None),
        P("dp", None, "head"),
        P("dp", None),
    )
    out_specs = (P("dp", "head"), P("dp", None, "head", None), P("dp", None, "head"), P("dp", None))
    return jax.shard_map(body, mesh=mesh, in_specs=in_specs, out_specs=out_specs, check_vma=False)
```

```python
import math

import jax
import jax.numpy as jnp
import numpy as np
from jax import lax
from jax.experimental import pallas as pl
from jax.experimental.pallas import tpu as pltpu
from jax.sharding import PartitionSpec as P

H = 8
DK = 256
DV = 512
EPSILON = 1e-06
F32 = jnp.float32
BF16 = jnp.bfloat16
STATS = 8


CHUNKS = 3
ORDER = [21 ^ k for k in (*range(0, 32, 2), *range(1, 32, 2))]
SLOT = [ORDER.index(k) for k in range(32)]
SPREAD_FLOPS = 10_000_000_000


def exchange(pieces):
    return lax.all_to_all(pieces, "head", 0, 0, tiled=True, axis_index_groups=[ORDER])


def dot_last(left, right):
    return lax.dot_general(left, right, (((1,), (1,)), ((), ())), preferred_element_type=F32)


def dot(left, right):
    return jnp.dot(left, right, preferred_element_type=F32)


def column(row):
    n = row.shape[1]
    at_row = lax.broadcasted_iota(jnp.int32, (n, n), 0)
    at_col = lax.broadcasted_iota(jnp.int32, (n, n), 1)
    return jnp.sum(jnp.where(at_row == at_col, row, 0.0), axis=1, keepdims=True)


def split_hi_lo(value):
    high = value.astype(BF16).astype(F32)
    return high, value - high


def repeat_matrix(rows, batch):
    spread = 2 * rows * batch
    col = np.arange(H * spread)
    return jnp.asarray(np.arange(H * rows)[:, None] == col // spread * rows + col % rows, BF16)


def own_mask(rows, batch):
    row = np.arange(4 * batch)[:, None]
    col = np.arange(2 * rows * batch)
    return jnp.asarray((row % batch == col // (2 * rows)) & (row // (2 * batch) == col // rows % 2), BF16)


def spread_kernel(in_ref, out_ref):
    value = in_ref[...]
    for j in range(out_ref.shape[0]):
        out_ref[j] = value


def project_kernel(
    x_ref, gain_ref, wi_ref, wf_ref, bi_ref, bf_ref, nrm_ref, stab_ref, wq_ref, wk_ref, wv_ref, wg_ref, mem_ref,
    repeat_ref, own_ref,
    out_ref, nrm_out_ref, stab_out_ref, f_rows_ref, ik_rows_ref, sum_scale_ref, own_value_ref, floor_ref,
    xn_ref, tail_ref, fg_ref, ig_ref,
):
    pieces, batch, width = x_ref.shape
    half = batch // 2
    rows = wq_ref.shape[0] // H
    total = jnp.zeros((batch, width), F32)
    for j in range(pieces):
        x = x_ref[j].astype(F32)
        total = total + x * x
    mean = jnp.sum(total, axis=1, keepdims=True) / (pieces * width)
    scale = lax.rsqrt(mean + EPSILON)
    tail_ref[...] = jnp.zeros(tail_ref.shape, F32)
    for j in range(pieces):
        cut = slice(ORDER[j] * width, (ORDER[j] + 1) * width)
        xn_ref[:, cut] = (x_ref[j].astype(F32) * scale * gain_ref[:, cut]).astype(BF16)
    x_norm = xn_ref[...]

    left = jnp.concatenate([wq_ref[...], wk_ref[...], wi_ref[...], wf_ref[...]], axis=0)
    mixed = dot_last(left, x_norm)
    query_t = mixed[: H * rows]
    key_t = mixed[H * rows : 2 * H * rows] / math.sqrt(DK)
    input_pre = mixed[2 * H * rows : 2 * H * rows + H] + column(bi_ref[...])
    forget_pre = mixed[2 * H * rows + H :] + column(bf_ref[...])
    log_forget = jnp.minimum(forget_pre, 0.0) - jnp.log1p(jnp.exp(-jnp.abs(forget_pre)))
    kept = log_forget + stab_ref[...]
    stab_new = jnp.maximum(kept, input_pre)
    input_gate = jnp.exp(input_pre - stab_new)
    forget_gate = jnp.exp(kept - stab_new)
    stab_out_ref[...] = stab_new
    fg_ref[...] = forget_gate
    ig_ref[...] = input_gate

    for h in range(H):
        part = slice(h * rows, (h + 1) * rows)
        key_h = key_t[part]
        query_h = query_t[part]
        f_h = jnp.broadcast_to(forget_gate[h : h + 1], (rows, batch))
        ik_h = input_gate[h : h + 1] * key_h
        norm_h = f_h * nrm_ref[part] + ik_h
        nrm_out_ref[part] = norm_h
        f_rows_ref[part] = f_h
        ik_rows_ref[part] = ik_h
        norm_query = jnp.sum(norm_h * query_h, axis=0, keepdims=True)
        key_query = jnp.sum(key_h * query_h, axis=0, keepdims=True)
        kinds = (*split_hi_lo(norm_query), *split_hi_lo(key_query))
        for k, kind in enumerate(kinds):
            for core in range(2):
                tail_ref[core, h, 4 + k : 5 + k, :batch] = kind

    spread = batch * rows
    high, low = split_hi_lo(query_t.T)
    both = jnp.concatenate([high, low], axis=0).astype(BF16)
    spread = repeat_ref.shape[1] // H
    wide = dot(both, repeat_ref[...]).astype(BF16)
    share = pieces // H
    deep = 2 * rows
    for h in range(H):
        wide_h = wide[:, h * spread : (h + 1) * spread]
        left = jnp.concatenate([wide_h, wide_h], axis=0) * own_ref[...]
        right = [mem_ref[:, h, k * deep : (k + 1) * deep].reshape(spread, width) for k in range(2)]
        product = dot(left, jnp.concatenate(right, axis=1))
        for parity in range(2):
            at = parity * 2 * batch
            numer = (product[at : at + batch] + product[at + batch : at + 2 * batch]).astype(BF16)
            for k in range(2):
                out_ref[SLOT[h * share + 2 * k + parity], :batch] = numer[:, k * width : (k + 1) * width]

    value_gate = dot(x_norm, jnp.concatenate([wv_ref[...], wg_ref[...]], axis=1))
    value = value_gate[:, :width]
    for core in range(2):
        first = value[core * half : core * half + 8].astype(BF16)
        rest = value[core * half + 8 : (core + 1) * half]
        for h in range(H):
            tail_ref[core, h, :4] = rest
        for j in range(core, pieces, 2):
            out_ref[SLOT[j], batch : batch + 8] = first
            out_ref[SLOT[j], batch + 8 :] = tail_ref[core, j // share].astype(BF16)

    head = lax.axis_index("head") * width // DV
    pick = lambda ref: column(ref[pl.ds(head, 1), :])
    gate = jax.nn.sigmoid(value_gate[:, width:])
    sum_scale_ref[...] = gate * pick(fg_ref)
    own_value_ref[...] = gate * (pick(ig_ref) * value.astype(BF16).astype(F32))
    floor_ref[...] = jnp.broadcast_to(jnp.exp(-pick(stab_out_ref)), floor_ref.shape)


def output_kernel(in_ref, sum_scale_ref, own_ref, floor_ref, wo_ref, out_ref):
    pieces, batch, width = out_ref.shape
    total = in_ref[0, :batch].astype(F32)
    tail = in_ref[0, batch + 8 :].astype(F32)
    for j in range(1, pieces):
        total = total + in_ref[j, :batch].astype(F32)
        tail = tail + in_ref[j, batch + 8 :].astype(F32)
    norm_query = column(tail[4:5, :batch] + tail[5:6, :batch])
    key_query = column(tail[6:7, :batch] + tail[7:8, :batch])
    numer = sum_scale_ref[...] * total + own_ref[...] * key_query
    hidden = (numer / jnp.maximum(jnp.abs(norm_query), floor_ref[...])).astype(BF16)
    for j in range(0, pieces, 2):
        pair = dot(hidden, wo_ref[:, j * width : (j + 2) * width]).astype(BF16)
        out_ref[SLOT[j]] = pair[:, :width]
        out_ref[SLOT[j + 1]] = pair[:, width:]


def memory_half(side, f_rows_ref, ik_rows_ref, half_ref, mem_ref, out_hbm, wide_ref, new_ref, sems):
    pieces, depth, width = half_ref.shape
    _, _, rows, _ = mem_ref.shape
    half = wide_ref.shape[1]
    share = pieces // H
    first = depth - 16
    lower = lax.axis_index("head") % 2 == side
    base = jnp.where(lower, 0, half)
    for j in range(pieces):
        cut = slice((j % share) * width, (j % share + 1) * width)
        wide_ref[j // share, :, cut] = half_ref[SLOT[j], first:].astype(F32)[:half]

    f_mine = jnp.where(lower, f_rows_ref[:, :half], f_rows_ref[:, half:])
    ik_mine = jnp.where(lower, ik_rows_ref[:, :half], ik_rows_ref[:, half:])
    step = half // CHUNKS
    copies = []
    for k in range(CHUNKS):
        for h in range(H):
            part = slice(h * rows, (h + 1) * rows)
            for i in range(k * step, (k + 1) * step):
                kept = f_mine[part, i : i + 1] * mem_ref[base + i, h].astype(F32)
                added = ik_mine[part, i : i + 1] * wide_ref[h, i : i + 1, :]
                new_ref[i, h] = (kept + added).astype(BF16)
        source = new_ref.at[k * step : (k + 1) * step]
        target = out_hbm.at[pl.ds(base + k * step, step)]
        copies.append(pltpu.make_async_copy(source, target, sems.at[k]))
        copies[-1].start()
    for copy in copies:
        copy.wait()


def memory_mine_kernel(
    f_rows_ref, ik_rows_ref, norm_ref, stab_ref, half_ref, mem_ref,
    out_hbm, norm_out_hbm, stab_out_hbm, wide_ref, new_ref, sems, small_sems,
):
    norm_copy = pltpu.make_async_copy(norm_ref, norm_out_hbm, small_sems.at[0])
    stab_copy = pltpu.make_async_copy(stab_ref, stab_out_hbm, small_sems.at[1])
    norm_copy.start()
    stab_copy.start()
    memory_half(0, f_rows_ref, ik_rows_ref, half_ref, mem_ref, out_hbm, wide_ref, new_ref, sems)
    norm_copy.wait()
    stab_copy.wait()


def memory_other_kernel(
    f_rows_ref, ik_rows_ref, half_ref, mem_ref, partial_hbm, out_hbm, wide_ref, new_ref, sems
):
    del partial_hbm
    memory_half(1, f_rows_ref, ik_rows_ref, half_ref, mem_ref, out_hbm, wide_ref, new_ref, sems)


def finish_kernel(in_ref, residual_ref, out_ref):
    total = residual_ref[...]
    acc = in_ref[0].astype(F32)
    for j in range(1, in_ref.shape[0]):
        acc = acc + in_ref[j].astype(F32)
    out_ref[...] = total + acc


def call(kernel, outs, n_in, scratch=(), flops=1_000_000, hbm_out=False, alias=False):
    vmem, hbm = (pl.BlockSpec(memory_space=space) for space in (pltpu.VMEM, pltpu.HBM))
    return pl.pallas_call(
        kernel,
        out_shape=[jax.ShapeDtypeStruct(*out) for out in outs],
        in_specs=[vmem] * n_in + [hbm] * alias,
        out_specs=[hbm if hbm_out else vmem] * len(outs),
        scratch_shapes=list(scratch),
        input_output_aliases={n_in: 0} if alias else {},
        compiler_params=pltpu.CompilerParams(vmem_limit_bytes=16 * 2**20),
        cost_estimate=pl.CostEstimate(flops=flops, bytes_accessed=2_000_000, transcendentals=0),
    )


def body(
    residual,
    norm_gain,
    w_query,
    w_key,
    w_value,
    w_gate,
    w_input,
    w_forget,
    b_input,
    b_forget,
    w_out,
    memory,
    normalizer,
    stabilizer,
):
    count = lax.axis_size("head")
    batch, width = residual.shape
    rows = w_query.shape[1]
    features = count * width
    (pieces,) = call(spread_kernel, [((count, batch, width), BF16)], 1, flops=SPREAD_FLOPS)(
        residual.astype(BF16)
    )
    gathered = exchange(pieces)

    piece = ((count, batch, width), BF16)
    sources = (
        norm_gain[None],
        w_input,
        w_forget,
        b_input[None],
        b_forget[None],
        normalizer.transpose(1, 2, 0).reshape(H * rows, batch),
        stabilizer.T,
        w_query.reshape(H * rows, features),
        w_key.reshape(H * rows, features),
        w_value,
        w_gate,
        memory.reshape(batch, H, rows, DV // width, width)
        .transpose(0, 1, 3, 2, 4)
        .reshape(batch, H, DV // width * rows, width),
        repeat_matrix(rows, batch),
        own_mask(rows, batch),
    )
    payload, norm_new, stab_new, f_rows, ik_rows, sum_scale, own, floor = call(
        project_kernel,
        [
            ((count, batch + batch // 2 + 4, width), BF16),
            ((H * rows, batch), F32),
            ((H, batch), F32),
            ((H * rows, batch), F32),
            ((H * rows, batch), F32),
            ((batch, width), F32),
            ((batch, width), F32),
            ((batch, width), F32),
        ],
        1 + len(sources),
        scratch=[
            pltpu.VMEM((batch, features), BF16),
            pltpu.VMEM((2, H, 8, width), F32),
            pltpu.VMEM((H, batch), F32),
            pltpu.VMEM((H, batch), F32),
        ],
        flops=100_000_000,
    )(gathered, *sources)
    arrived = exchange(payload)
    (branch,) = call(output_kernel, [piece], 5, flops=30_000_000)(
        arrived, sum_scale, own, floor, w_out
    )
    returned = exchange(branch)
    with jax.named_scope("swap"):
        other = lax.ppermute(arrived[:, batch:], "head", [(i, i ^ 1) for i in range(count)])
    half_scratch = [
        pltpu.VMEM((H, batch // 2, DV), F32),
        pltpu.VMEM((batch // 2, *memory.shape[1:]), BF16),
        pltpu.SemaphoreType.DMA((CHUNKS,)),
    ]
    mem_half, norm_out, stab_out = call(
        memory_mine_kernel,
        [(memory.shape, BF16), ((H * rows, batch), F32), ((H, batch), F32)],
        6,
        scratch=[*half_scratch, pltpu.SemaphoreType.DMA((2,))],
        flops=50_000_000,
        hbm_out=True,
    )(f_rows, ik_rows, norm_new, stab_new, arrived, memory)
    (mem_new,) = call(
        memory_other_kernel,
        [(memory.shape, BF16)],
        4,
        scratch=half_scratch,
        flops=50_000_000,
        hbm_out=True,
        alias=True,
    )(f_rows, ik_rows, other, memory, mem_half)
    (res_out,) = call(finish_kernel, [((batch, width), F32)], 2)(returned, residual)
    norm_out = norm_out.reshape(H, rows, batch).transpose(2, 0, 1)
    return res_out, mem_new, norm_out, stab_out.T


def solution(mesh):
    in_specs = (
        P("dp", "head"),
        P(),
        P(None, "head", None),
        P(None, "head", None),
        P(None, "head"),
        P(None, "head"),
        P(),
        P(),
        P(),
        P(),
        P("head", None),
        P("dp", None, "head", None),
        P("dp", None, "head"),
        P("dp", None),
    )
    out_specs = (P("dp", "head"), P("dp", None, "head", None), P("dp", None, "head"), P("dp", None))
    return jax.shard_map(body, mesh=mesh, in_specs=in_specs, out_specs=out_specs, check_vma=False)
```

```python
import math

import jax
import jax.numpy as jnp
import numpy as np
from jax import lax
from jax.experimental import pallas as pl
from jax.experimental.pallas import tpu as pltpu
from jax.sharding import PartitionSpec as P

H = 8
DK = 256
DV = 512
EPSILON = 1e-06
F32 = jnp.float32
BF16 = jnp.bfloat16
STATS = 8


CHUNKS = 3
ORDER = [21 ^ k for k in (*range(0, 32, 2), *range(1, 32, 2))]
SLOT = [ORDER.index(k) for k in range(32)]
SPREAD_FLOPS = 10_000_000_000


def exchange(pieces):
    return lax.all_to_all(pieces, "head", 0, 0, tiled=True, axis_index_groups=[ORDER])


def dot_last(left, right):
    return lax.dot_general(left, right, (((1,), (1,)), ((), ())), preferred_element_type=F32)


def dot(left, right):
    return jnp.dot(left, right, preferred_element_type=F32)


def column(row):
    n = row.shape[1]
    at_row = lax.broadcasted_iota(jnp.int32, (n, n), 0)
    at_col = lax.broadcasted_iota(jnp.int32, (n, n), 1)
    return jnp.sum(jnp.where(at_row == at_col, row, 0.0), axis=1, keepdims=True)


def split_hi_lo(value):
    high = value.astype(BF16).astype(F32)
    return high, value - high


def repeat_matrix(rows, batch):
    spread = 2 * rows * batch
    col = np.arange(H * spread)
    return jnp.asarray(np.arange(H * rows)[:, None] == col // spread * rows + col % rows, BF16)


def own_mask(rows, batch):
    row = np.arange(4 * batch)[:, None]
    col = np.arange(2 * rows * batch)
    return jnp.asarray((row % batch == col // (2 * rows)) & (row // (2 * batch) == col // rows % 2), BF16)


def spread_kernel(in_ref, out_ref):
    value = in_ref[...].astype(BF16)
    for j in range(out_ref.shape[0]):
        out_ref[j] = value


def project_kernel(
    x_ref, gain_ref, wi_ref, wf_ref, bi_ref, bf_ref, nrm_ref, stab_ref, wq_ref, wk_ref, wv_ref, wg_ref, mem_ref,
    repeat_ref, own_ref,
    out_ref, nrm_out_ref, stab_out_ref, f_rows_ref, ik_rows_ref, sum_scale_ref, own_value_ref, floor_ref,
    xn_ref, tail_ref, fg_ref, ig_ref,
):
    pieces, batch, width = x_ref.shape
    half = batch // 2
    rows = wq_ref.shape[0] // H
    total = jnp.zeros((batch, width), F32)
    for j in range(pieces):
        x = x_ref[j].astype(F32)
        total = total + x * x
    mean = jnp.sum(total, axis=1, keepdims=True) / (pieces * width)
    scale = lax.rsqrt(mean + EPSILON)
    tail_ref[...] = jnp.zeros(tail_ref.shape, F32)
    for j in range(pieces):
        cut = slice(ORDER[j] * width, (ORDER[j] + 1) * width)
        xn_ref[:, cut] = (x_ref[j].astype(F32) * scale * gain_ref[:, cut]).astype(BF16)
    x_norm = xn_ref[...]

    value_gate = dot(x_norm, jnp.concatenate([wv_ref[...], wg_ref[...]], axis=1))
    left = jnp.concatenate([wq_ref[...], wk_ref[...], wi_ref[...], wf_ref[...]], axis=0)
    mixed = dot_last(left, x_norm)
    query_t = mixed[: H * rows]
    key_t = mixed[H * rows : 2 * H * rows] / math.sqrt(DK)
    input_pre = mixed[2 * H * rows : 2 * H * rows + H] + column(bi_ref[...])
    forget_pre = mixed[2 * H * rows + H :] + column(bf_ref[...])
    log_forget = jnp.minimum(forget_pre, 0.0) - jnp.log1p(jnp.exp(-jnp.abs(forget_pre)))
    kept = log_forget + stab_ref[...]
    stab_new = jnp.maximum(kept, input_pre)
    input_gate = jnp.exp(input_pre - stab_new)
    forget_gate = jnp.exp(kept - stab_new)
    stab_out_ref[...] = stab_new
    fg_ref[...] = forget_gate
    ig_ref[...] = input_gate

    for h in range(H):
        part = slice(h * rows, (h + 1) * rows)
        key_h = key_t[part]
        query_h = query_t[part]
        f_h = jnp.broadcast_to(forget_gate[h : h + 1], (rows, batch))
        ik_h = input_gate[h : h + 1] * key_h
        norm_h = f_h * nrm_ref[part] + ik_h
        nrm_out_ref[part] = norm_h
        f_rows_ref[part] = f_h
        ik_rows_ref[part] = ik_h
        norm_query = jnp.sum(norm_h * query_h, axis=0, keepdims=True)
        key_query = jnp.sum(key_h * query_h, axis=0, keepdims=True)
        kinds = (*split_hi_lo(norm_query), *split_hi_lo(key_query))
        for k, kind in enumerate(kinds):
            for core in range(2):
                tail_ref[core, h, 4 + k : 5 + k, :batch] = kind

    spread = batch * rows
    high, low = split_hi_lo(query_t.T)
    both = jnp.concatenate([high, low], axis=0).astype(BF16)
    spread = repeat_ref.shape[1] // H
    wide = dot(both, repeat_ref[...]).astype(BF16)
    share = pieces // H
    deep = 2 * rows
    for h in range(H):
        wide_h = wide[:, h * spread : (h + 1) * spread]
        left = jnp.concatenate([wide_h, wide_h], axis=0) * own_ref[...]
        right = [mem_ref[:, h, k * deep : (k + 1) * deep].reshape(spread, width) for k in range(2)]
        product = dot(left, jnp.concatenate(right, axis=1))
        for parity in range(2):
            at = parity * 2 * batch
            numer = (product[at : at + batch] + product[at + batch : at + 2 * batch]).astype(BF16)
            for k in range(2):
                out_ref[SLOT[h * share + 2 * k + parity], :batch] = numer[:, k * width : (k + 1) * width]

    value = value_gate[:, :width]
    for core in range(2):
        first = value[core * half : core * half + 8].astype(BF16)
        rest = value[core * half + 8 : (core + 1) * half]
        for h in range(H):
            tail_ref[core, h, :4] = rest
        for j in range(core, pieces, 2):
            out_ref[SLOT[j], batch : batch + 8] = first
            out_ref[SLOT[j], batch + 8 :] = tail_ref[core, j // share].astype(BF16)

    head = lax.axis_index("head") * width // DV
    pick = lambda ref: column(ref[pl.ds(head, 1), :])
    gate = jax.nn.sigmoid(value_gate[:, width:])
    sum_scale_ref[...] = gate * pick(fg_ref)
    own_value_ref[...] = gate * (pick(ig_ref) * value.astype(BF16).astype(F32))
    floor_ref[...] = jnp.broadcast_to(jnp.exp(-pick(stab_out_ref)), floor_ref.shape)


def output_kernel(in_ref, sum_scale_ref, own_ref, floor_ref, wo_ref, out_ref):
    pieces, batch, width = out_ref.shape
    total = in_ref[0, :batch].astype(F32)
    tail = in_ref[0, batch + 8 :].astype(F32)
    for j in range(1, pieces):
        total = total + in_ref[j, :batch].astype(F32)
        tail = tail + in_ref[j, batch + 8 :].astype(F32)
    norm_query = column(tail[4:5, :batch] + tail[5:6, :batch])
    key_query = column(tail[6:7, :batch] + tail[7:8, :batch])
    numer = sum_scale_ref[...] * total + own_ref[...] * key_query
    hidden = (numer / jnp.maximum(jnp.abs(norm_query), floor_ref[...])).astype(BF16)
    for j in range(0, pieces, 2):
        pair = dot(hidden, wo_ref[:, j * width : (j + 2) * width]).astype(BF16)
        out_ref[SLOT[j]] = pair[:, :width]
        out_ref[SLOT[j + 1]] = pair[:, width:]


def memory_half(side, f_rows_ref, ik_rows_ref, half_ref, mem_ref, out_hbm, wide_ref, new_ref, sems):
    pieces, depth, width = half_ref.shape
    _, _, rows, _ = mem_ref.shape
    half = wide_ref.shape[1]
    share = pieces // H
    first = depth - 16
    lower = lax.axis_index("head") % 2 == side
    base = jnp.where(lower, 0, half)
    for j in range(pieces):
        cut = slice((j % share) * width, (j % share + 1) * width)
        wide_ref[j // share, :, cut] = half_ref[SLOT[j], first:].astype(F32)[:half]

    f_mine = jnp.where(lower, f_rows_ref[:, :half], f_rows_ref[:, half:])
    ik_mine = jnp.where(lower, ik_rows_ref[:, :half], ik_rows_ref[:, half:])
    step = half // CHUNKS
    copies = []
    for k in range(CHUNKS):
        for h in range(H):
            part = slice(h * rows, (h + 1) * rows)
            for i in range(k * step, (k + 1) * step):
                kept = f_mine[part, i : i + 1] * mem_ref[base + i, h].astype(F32)
                added = ik_mine[part, i : i + 1] * wide_ref[h, i : i + 1, :]
                new_ref[i, h] = (kept + added).astype(BF16)
        source = new_ref.at[k * step : (k + 1) * step]
        target = out_hbm.at[pl.ds(base + k * step, step)]
        copies.append(pltpu.make_async_copy(source, target, sems.at[k]))
        copies[-1].start()
    for copy in copies:
        copy.wait()


def memory_mine_kernel(
    f_rows_ref, ik_rows_ref, norm_ref, stab_ref, half_ref, mem_ref,
    out_hbm, norm_out_hbm, stab_out_hbm, wide_ref, new_ref, sems, small_sems,
):
    norm_copy = pltpu.make_async_copy(norm_ref, norm_out_hbm, small_sems.at[0])
    stab_copy = pltpu.make_async_copy(stab_ref, stab_out_hbm, small_sems.at[1])
    norm_copy.start()
    stab_copy.start()
    memory_half(0, f_rows_ref, ik_rows_ref, half_ref, mem_ref, out_hbm, wide_ref, new_ref, sems)
    norm_copy.wait()
    stab_copy.wait()


def memory_other_kernel(
    f_rows_ref, ik_rows_ref, half_ref, mem_ref, partial_hbm, out_hbm, wide_ref, new_ref, sems
):
    del partial_hbm
    memory_half(1, f_rows_ref, ik_rows_ref, half_ref, mem_ref, out_hbm, wide_ref, new_ref, sems)


def finish_kernel(in_ref, residual_ref, out_ref):
    total = residual_ref[...]
    acc = in_ref[0].astype(F32)
    for j in range(1, in_ref.shape[0]):
        acc = acc + in_ref[j].astype(F32)
    out_ref[...] = total + acc


def call(kernel, outs, n_in, scratch=(), flops=1_000_000, hbm_out=False, alias=False):
    vmem, hbm = (pl.BlockSpec(memory_space=space) for space in (pltpu.VMEM, pltpu.HBM))
    return pl.pallas_call(
        kernel,
        out_shape=[jax.ShapeDtypeStruct(*out) for out in outs],
        in_specs=[vmem] * n_in + [hbm] * alias,
        out_specs=[hbm if hbm_out else vmem] * len(outs),
        scratch_shapes=list(scratch),
        input_output_aliases={n_in: 0} if alias else {},
        compiler_params=pltpu.CompilerParams(vmem_limit_bytes=16 * 2**20),
        cost_estimate=pl.CostEstimate(flops=flops, bytes_accessed=2_000_000, transcendentals=0),
    )


def body(
    residual,
    norm_gain,
    w_query,
    w_key,
    w_value,
    w_gate,
    w_input,
    w_forget,
    b_input,
    b_forget,
    w_out,
    memory,
    normalizer,
    stabilizer,
):
    count = lax.axis_size("head")
    batch, width = residual.shape
    rows = w_query.shape[1]
    features = count * width
    (pieces,) = call(spread_kernel, [((count, batch, width), BF16)], 1, flops=SPREAD_FLOPS)(residual)
    gathered = exchange(pieces)

    piece = ((count, batch, width), BF16)
    sources = (
        norm_gain[None],
        w_input,
        w_forget,
        b_input[None],
        b_forget[None],
        normalizer.transpose(1, 2, 0).reshape(H * rows, batch),
        stabilizer.T,
        w_query.reshape(H * rows, features),
        w_key.reshape(H * rows, features),
        w_value,
        w_gate,
        memory.reshape(batch, H, rows, DV // width, width)
        .transpose(0, 1, 3, 2, 4)
        .reshape(batch, H, DV // width * rows, width),
        repeat_matrix(rows, batch),
        own_mask(rows, batch),
    )
    payload, norm_new, stab_new, f_rows, ik_rows, sum_scale, own, floor = call(
        project_kernel,
        [
            ((count, batch + batch // 2 + 4, width), BF16),
            ((H * rows, batch), F32),
            ((H, batch), F32),
            ((H * rows, batch), F32),
            ((H * rows, batch), F32),
            ((batch, width), F32),
            ((batch, width), F32),
            ((batch, width), F32),
        ],
        1 + len(sources),
        scratch=[
            pltpu.VMEM((batch, features), BF16),
            pltpu.VMEM((2, H, 8, width), F32),
            pltpu.VMEM((H, batch), F32),
            pltpu.VMEM((H, batch), F32),
        ],
        flops=100_000_000,
    )(gathered, *sources)
    arrived = exchange(payload)
    (branch,) = call(output_kernel, [piece], 5, flops=30_000_000)(
        arrived, sum_scale, own, floor, w_out
    )
    returned = exchange(branch)
    with jax.named_scope("swap"):
        other = lax.ppermute(arrived[:, batch:], "head", [(i, i ^ 1) for i in range(count)])
    half_scratch = [
        pltpu.VMEM((H, batch // 2, DV), F32),
        pltpu.VMEM((batch // 2, *memory.shape[1:]), BF16),
        pltpu.SemaphoreType.DMA((CHUNKS,)),
    ]
    mem_half, norm_out, stab_out = call(
        memory_mine_kernel,
        [(memory.shape, BF16), ((H * rows, batch), F32), ((H, batch), F32)],
        6,
        scratch=[*half_scratch, pltpu.SemaphoreType.DMA((2,))],
        flops=50_000_000,
        hbm_out=True,
    )(f_rows, ik_rows, norm_new, stab_new, arrived, memory)
    (mem_new,) = call(
        memory_other_kernel,
        [(memory.shape, BF16)],
        4,
        scratch=half_scratch,
        flops=50_000_000,
        hbm_out=True,
        alias=True,
    )(f_rows, ik_rows, other, memory, mem_half)
    (res_out,) = call(finish_kernel, [((batch, width), F32)], 2)(returned, residual)
    norm_out = norm_out.reshape(H, rows, batch).transpose(2, 0, 1)
    return res_out, mem_new, norm_out, stab_out.T


def solution(mesh):
    in_specs = (
        P("dp", "head"),
        P(),
        P(None, "head", None),
        P(None, "head", None),
        P(None, "head"),
        P(None, "head"),
        P(),
        P(),
        P(),
        P(),
        P("head", None),
        P("dp", None, "head", None),
        P("dp", None, "head"),
        P("dp", None),
    )
    out_specs = (P("dp", "head"), P("dp", None, "head", None), P("dp", None, "head"), P("dp", None))
    return jax.shard_map(body, mesh=mesh, in_specs=in_specs, out_specs=out_specs, check_vma=False)
```

```python
import math

import jax
import jax.numpy as jnp
import numpy as np
from jax import lax
from jax.experimental import pallas as pl
from jax.experimental.pallas import tpu as pltpu
from jax.sharding import PartitionSpec as P

H = 8
DK = 256
DV = 512
EPSILON = 1e-06
F32 = jnp.float32
BF16 = jnp.bfloat16
STATS = 8


CHUNKS = 3
ORDER = [21 ^ k for k in (*range(0, 32, 2), *range(1, 32, 2))]
SLOT = [ORDER.index(k) for k in range(32)]
SPREAD_FLOPS = 10_000_000_000


def exchange(pieces):
    return lax.all_to_all(pieces, "head", 0, 0, tiled=True, axis_index_groups=[ORDER])


def dot_last(left, right):
    return lax.dot_general(left, right, (((1,), (1,)), ((), ())), preferred_element_type=F32)


def dot(left, right):
    return jnp.dot(left, right, preferred_element_type=F32)


def column(row):
    n = row.shape[1]
    at_row = lax.broadcasted_iota(jnp.int32, (n, n), 0)
    at_col = lax.broadcasted_iota(jnp.int32, (n, n), 1)
    return jnp.sum(jnp.where(at_row == at_col, row, 0.0), axis=1, keepdims=True)


def split_hi_lo(value):
    high = value.astype(BF16).astype(F32)
    return high, value - high


def repeat_matrix(rows, batch):
    spread = 2 * rows * batch
    col = np.arange(H * spread)
    return jnp.asarray(np.arange(H * rows)[:, None] == col // spread * rows + col % rows, BF16)


def own_mask(rows, batch):
    row = np.arange(4 * batch)[:, None]
    col = np.arange(2 * rows * batch)
    return jnp.asarray((row % batch == col // (2 * rows)) & (row // (2 * batch) == col // rows % 2), BF16)


def spread_kernel(in_ref, out_ref):
    value = in_ref[...]
    for j in range(out_ref.shape[0]):
        out_ref[j] = value


def project_kernel(
    x_ref, gain_ref, wi_ref, wf_ref, bi_ref, bf_ref, nrm_ref, stab_ref, wq_ref, wk_ref, wv_ref, wg_ref, mem_ref,
    repeat_ref, own_ref,
    out_ref, nrm_out_ref, stab_out_ref, f_rows_ref, ik_rows_ref, sum_scale_ref, own_value_ref, floor_ref,
    xn_ref, tail_ref, fg_ref, ig_ref,
):
    pieces, batch, width = x_ref.shape
    half = batch // 2
    rows = wq_ref.shape[0] // H
    total = jnp.zeros((batch, width), F32)
    for j in range(pieces):
        x = x_ref[j].astype(F32)
        total = total + x * x
    mean = jnp.sum(total, axis=1, keepdims=True) / (pieces * width)
    scale = lax.rsqrt(mean + EPSILON)
    tail_ref[...] = jnp.zeros(tail_ref.shape, F32)
    for j in range(pieces):
        cut = slice(ORDER[j] * width, (ORDER[j] + 1) * width)
        xn_ref[:, cut] = (x_ref[j].astype(F32) * scale * gain_ref[:, cut]).astype(BF16)
    x_norm = xn_ref[...]

    value_gate = dot(x_norm, jnp.concatenate([wv_ref[...], wg_ref[...]], axis=1))
    left = jnp.concatenate([wq_ref[...], wk_ref[...], wi_ref[...], wf_ref[...]], axis=0)
    mixed = dot_last(left, x_norm)
    query_t = mixed[: H * rows]
    key_t = mixed[H * rows : 2 * H * rows] / math.sqrt(DK)
    input_pre = mixed[2 * H * rows : 2 * H * rows + H] + column(bi_ref[...])
    forget_pre = mixed[2 * H * rows + H :] + column(bf_ref[...])
    log_forget = jnp.minimum(forget_pre, 0.0) - jnp.log1p(jnp.exp(-jnp.abs(forget_pre)))
    kept = log_forget + stab_ref[...]
    stab_new = jnp.maximum(kept, input_pre)
    input_gate = jnp.exp(input_pre - stab_new)
    forget_gate = jnp.exp(kept - stab_new)
    stab_out_ref[...] = stab_new
    fg_ref[...] = forget_gate
    ig_ref[...] = input_gate

    for h in range(H):
        part = slice(h * rows, (h + 1) * rows)
        key_h = key_t[part]
        query_h = query_t[part]
        f_h = jnp.broadcast_to(forget_gate[h : h + 1], (rows, batch))
        ik_h = input_gate[h : h + 1] * key_h
        norm_h = f_h * nrm_ref[part] + ik_h
        nrm_out_ref[part] = norm_h
        f_rows_ref[part] = f_h
        ik_rows_ref[part] = ik_h
        norm_query = jnp.sum(norm_h * query_h, axis=0, keepdims=True)
        key_query = jnp.sum(key_h * query_h, axis=0, keepdims=True)
        kinds = (*split_hi_lo(norm_query), *split_hi_lo(key_query))
        for k, kind in enumerate(kinds):
            for core in range(2):
                tail_ref[core, h, 4 + k : 5 + k, :batch] = kind

    spread = batch * rows
    high, low = split_hi_lo(query_t.T)
    both = jnp.concatenate([high, low], axis=0).astype(BF16)
    spread = repeat_ref.shape[1] // H
    wide = dot(both, repeat_ref[...]).astype(BF16)
    share = pieces // H
    deep = 2 * rows
    for h in range(H):
        wide_h = wide[:, h * spread : (h + 1) * spread]
        left = jnp.concatenate([wide_h, wide_h], axis=0) * own_ref[...]
        right = [mem_ref[:, h, k * deep : (k + 1) * deep].reshape(spread, width) for k in range(2)]
        product = dot(left, jnp.concatenate(right, axis=1))
        for parity in range(2):
            at = parity * 2 * batch
            numer = (product[at : at + batch] + product[at + batch : at + 2 * batch]).astype(BF16)
            for k in range(2):
                out_ref[SLOT[h * share + 2 * k + parity], :batch] = numer[:, k * width : (k + 1) * width]

    value = value_gate[:, :width]
    for core in range(2):
        first = value[core * half : core * half + 8].astype(BF16)
        rest = value[core * half + 8 : (core + 1) * half]
        for h in range(H):
            tail_ref[core, h, :4] = rest
        for j in range(core, pieces, 2):
            out_ref[SLOT[j], batch : batch + 8] = first
            out_ref[SLOT[j], batch + 8 :] = tail_ref[core, j // share].astype(BF16)

    head = lax.axis_index("head") * width // DV
    pick = lambda ref: column(ref[pl.ds(head, 1), :])
    gate = jax.nn.sigmoid(value_gate[:, width:])
    sum_scale_ref[...] = gate * pick(fg_ref)
    own_value_ref[...] = gate * (pick(ig_ref) * value.astype(BF16).astype(F32))
    floor_ref[...] = jnp.broadcast_to(jnp.exp(-pick(stab_out_ref)), floor_ref.shape)


def output_kernel(in_ref, sum_scale_ref, own_ref, floor_ref, wo_ref, out_ref):
    pieces, batch, width = out_ref.shape
    total = in_ref[0, :batch].astype(F32)
    tail = in_ref[0, batch + 8 :].astype(F32)
    for j in range(1, pieces):
        total = total + in_ref[j, :batch].astype(F32)
        tail = tail + in_ref[j, batch + 8 :].astype(F32)
    norm_query = column(tail[4:5, :batch] + tail[5:6, :batch])
    key_query = column(tail[6:7, :batch] + tail[7:8, :batch])
    numer = sum_scale_ref[...] * total + own_ref[...] * key_query
    hidden = (numer / jnp.maximum(jnp.abs(norm_query), floor_ref[...])).astype(BF16)
    for j in range(0, pieces, 2):
        pair = dot(hidden, wo_ref[:, j * width : (j + 2) * width]).astype(BF16)
        out_ref[SLOT[j]] = pair[:, :width]
        out_ref[SLOT[j + 1]] = pair[:, width:]


def memory_half(side, f_rows_ref, ik_rows_ref, half_ref, mem_ref, out_hbm, wide_ref, new_ref, sems):
    pieces, depth, width = half_ref.shape
    _, _, rows, _ = mem_ref.shape
    half = wide_ref.shape[1]
    share = pieces // H
    first = depth - 16
    lower = lax.axis_index("head") % 2 == side
    base = jnp.where(lower, 0, half)
    for j in range(pieces):
        cut = slice((j % share) * width, (j % share + 1) * width)
        wide_ref[j // share, :, cut] = half_ref[SLOT[j], first:].astype(F32)[:half]

    f_mine = jnp.where(lower, f_rows_ref[:, :half], f_rows_ref[:, half:])
    ik_mine = jnp.where(lower, ik_rows_ref[:, :half], ik_rows_ref[:, half:])
    step = half // CHUNKS
    copies = []
    for k in range(CHUNKS):
        for h in range(H):
            part = slice(h * rows, (h + 1) * rows)
            for i in range(k * step, (k + 1) * step):
                kept = f_mine[part, i : i + 1] * mem_ref[base + i, h].astype(F32)
                added = ik_mine[part, i : i + 1] * wide_ref[h, i : i + 1, :]
                new_ref[i, h] = (kept + added).astype(BF16)
        source = new_ref.at[k * step : (k + 1) * step]
        target = out_hbm.at[pl.ds(base + k * step, step)]
        copies.append(pltpu.make_async_copy(source, target, sems.at[k]))
        copies[-1].start()
    for copy in copies:
        copy.wait()


def memory_mine_kernel(
    f_rows_ref, ik_rows_ref, norm_ref, stab_ref, half_ref, mem_ref,
    out_hbm, norm_out_hbm, stab_out_hbm, wide_ref, new_ref, sems, small_sems,
):
    norm_copy = pltpu.make_async_copy(norm_ref, norm_out_hbm, small_sems.at[0])
    stab_copy = pltpu.make_async_copy(stab_ref, stab_out_hbm, small_sems.at[1])
    norm_copy.start()
    stab_copy.start()
    memory_half(0, f_rows_ref, ik_rows_ref, half_ref, mem_ref, out_hbm, wide_ref, new_ref, sems)
    norm_copy.wait()
    stab_copy.wait()


def memory_other_kernel(
    f_rows_ref, ik_rows_ref, half_ref, mem_ref, partial_hbm, out_hbm, wide_ref, new_ref, sems
):
    del partial_hbm
    memory_half(1, f_rows_ref, ik_rows_ref, half_ref, mem_ref, out_hbm, wide_ref, new_ref, sems)


def finish_kernel(in_ref, residual_ref, out_ref):
    total = residual_ref[...]
    acc = in_ref[0].astype(F32)
    for j in range(1, in_ref.shape[0]):
        acc = acc + in_ref[j].astype(F32)
    out_ref[...] = total + acc


def call(kernel, outs, n_in, scratch=(), flops=1_000_000, hbm_out=False, alias=False):
    vmem, hbm = (pl.BlockSpec(memory_space=space) for space in (pltpu.VMEM, pltpu.HBM))
    return pl.pallas_call(
        kernel,
        out_shape=[jax.ShapeDtypeStruct(*out) for out in outs],
        in_specs=[vmem] * n_in + [hbm] * alias,
        out_specs=[hbm if hbm_out else vmem] * len(outs),
        scratch_shapes=list(scratch),
        input_output_aliases={n_in: 0} if alias else {},
        compiler_params=pltpu.CompilerParams(vmem_limit_bytes=16 * 2**20),
        cost_estimate=pl.CostEstimate(flops=flops, bytes_accessed=2_000_000, transcendentals=0),
    )


def body(
    residual,
    norm_gain,
    w_query,
    w_key,
    w_value,
    w_gate,
    w_input,
    w_forget,
    b_input,
    b_forget,
    w_out,
    memory,
    normalizer,
    stabilizer,
):
    count = lax.axis_size("head")
    batch, width = residual.shape
    rows = w_query.shape[1]
    features = count * width
    (pieces,) = call(spread_kernel, [((count, batch, width), BF16)], 1, flops=SPREAD_FLOPS)(
        residual.astype(BF16)
    )
    gathered = exchange(pieces)

    piece = ((count, batch, width), BF16)
    sources = (
        norm_gain[None],
        w_input,
        w_forget,
        b_input[None],
        b_forget[None],
        normalizer.transpose(1, 2, 0).reshape(H * rows, batch),
        stabilizer.T,
        w_query.reshape(H * rows, features),
        w_key.reshape(H * rows, features),
        w_value,
        w_gate,
        memory.reshape(batch, H, rows, DV // width, width)
        .transpose(0, 1, 3, 2, 4)
        .reshape(batch, H, DV // width * rows, width),
        repeat_matrix(rows, batch),
        own_mask(rows, batch),
    )
    payload, norm_new, stab_new, f_rows, ik_rows, sum_scale, own, floor = call(
        project_kernel,
        [
            ((count, batch + batch // 2 + 4, width), BF16),
            ((H * rows, batch), F32),
            ((H, batch), F32),
            ((H * rows, batch), F32),
            ((H * rows, batch), F32),
            ((batch, width), F32),
            ((batch, width), F32),
            ((batch, width), F32),
        ],
        1 + len(sources),
        scratch=[
            pltpu.VMEM((batch, features), BF16),
            pltpu.VMEM((2, H, 8, width), F32),
            pltpu.VMEM((H, batch), F32),
            pltpu.VMEM((H, batch), F32),
        ],
        flops=100_000_000,
    )(gathered, *sources)
    arrived = exchange(payload)
    (branch,) = call(output_kernel, [piece], 5, flops=30_000_000)(
        arrived, sum_scale, own, floor, w_out
    )
    returned = exchange(branch)
    with jax.named_scope("swap"):
        other = lax.ppermute(arrived[:, batch:], "head", [(i, i ^ 1) for i in range(count)])
    half_scratch = [
        pltpu.VMEM((H, batch // 2, DV), F32),
        pltpu.VMEM((batch // 2, *memory.shape[1:]), BF16),
        pltpu.SemaphoreType.DMA((CHUNKS,)),
    ]
    mem_half, norm_out, stab_out = call(
        memory_mine_kernel,
        [(memory.shape, BF16), ((H * rows, batch), F32), ((H, batch), F32)],
        6,
        scratch=[*half_scratch, pltpu.SemaphoreType.DMA((2,))],
        flops=50_000_000,
        hbm_out=True,
    )(f_rows, ik_rows, norm_new, stab_new, arrived, memory)
    (mem_new,) = call(
        memory_other_kernel,
        [(memory.shape, BF16)],
        4,
        scratch=half_scratch,
        flops=50_000_000,
        hbm_out=True,
        alias=True,
    )(f_rows, ik_rows, other, memory, mem_half)
    (res_out,) = call(finish_kernel, [((batch, width), F32)], 2)(returned, residual)
    norm_out = norm_out.reshape(H, rows, batch).transpose(2, 0, 1)
    return res_out, mem_new, norm_out, stab_out.T


def solution(mesh):
    in_specs = (
        P("dp", "head"),
        P(),
        P(None, "head", None),
        P(None, "head", None),
        P(None, "head"),
        P(None, "head"),
        P(),
        P(),
        P(),
        P(),
        P("head", None),
        P("dp", None, "head", None),
        P("dp", None, "head"),
        P("dp", None),
    )
    out_specs = (P("dp", "head"), P("dp", None, "head", None), P("dp", None, "head"), P("dp", None))
    return jax.shard_map(body, mesh=mesh, in_specs=in_specs, out_specs=out_specs, check_vma=False)
```

```python
import math

import jax
import jax.numpy as jnp
import numpy as np
from jax import lax
from jax.experimental import pallas as pl
from jax.experimental.pallas import tpu as pltpu
from jax.sharding import PartitionSpec as P

H = 8
DK = 256
DV = 512
EPSILON = 1e-06
F32 = jnp.float32
BF16 = jnp.bfloat16
STATS = 8


CHUNKS = 3
ORDER = [21 ^ k for k in (*range(0, 32, 2), *range(1, 32, 2))]
SLOT = [ORDER.index(k) for k in range(32)]
SPREAD_FLOPS = 10_000_000_000


def exchange(pieces):
    return lax.all_to_all(pieces, "head", 0, 0, tiled=True, axis_index_groups=[ORDER])


def dot_last(left, right):
    return lax.dot_general(left, right, (((1,), (1,)), ((), ())), preferred_element_type=F32)


def dot(left, right):
    return jnp.dot(left, right, preferred_element_type=F32)


def column(row):
    n = row.shape[1]
    at_row = lax.broadcasted_iota(jnp.int32, (n, n), 0)
    at_col = lax.broadcasted_iota(jnp.int32, (n, n), 1)
    return jnp.sum(jnp.where(at_row == at_col, row, 0.0), axis=1, keepdims=True)


def split_hi_lo(value):
    high = value.astype(BF16).astype(F32)
    return high, value - high


def repeat_matrix(rows, batch):
    spread = 2 * rows * batch
    col = np.arange(H * spread)
    return jnp.asarray(np.arange(H * rows)[:, None] == col // spread * rows + col % rows, BF16)


def own_mask(rows, batch):
    row = np.arange(4 * batch)[:, None]
    col = np.arange(2 * rows * batch)
    return jnp.asarray((row % batch == col // (2 * rows)) & (row // (2 * batch) == col // rows % 2), BF16)


def spread_kernel(in_ref, out_ref):
    value = in_ref[...].astype(BF16)
    for j in range(out_ref.shape[0]):
        out_ref[j] = value


def project_kernel(
    x_ref, gain_ref, wi_ref, wf_ref, bi_ref, bf_ref, nrm_ref, stab_ref, wq_ref, wk_ref, wv_ref, wg_ref, mem_ref,
    repeat_ref, own_ref,
    out_ref, nrm_out_ref, stab_out_ref, f_rows_ref, ik_rows_ref, sum_scale_ref, own_value_ref, floor_ref,
    xn_ref, tail_ref, fg_ref, ig_ref,
):
    pieces, batch, width = x_ref.shape
    half = batch // 2
    rows = wq_ref.shape[0] // H
    total = jnp.zeros((batch, width), F32)
    for j in range(pieces):
        x = x_ref[j].astype(F32)
        total = total + x * x
    mean = jnp.sum(total, axis=1, keepdims=True) / (pieces * width)
    scale = lax.rsqrt(mean + EPSILON)
    tail_ref[...] = jnp.zeros(tail_ref.shape, F32)
    for j in range(pieces):
        cut = slice(ORDER[j] * width, (ORDER[j] + 1) * width)
        xn_ref[:, cut] = (x_ref[j].astype(F32) * scale * gain_ref[:, cut]).astype(BF16)
    x_norm = xn_ref[...]

    value_gate = dot(x_norm, jnp.concatenate([wv_ref[...], wg_ref[...]], axis=1))
    left = jnp.concatenate([wq_ref[...], wk_ref[...], wi_ref[...], wf_ref[...]], axis=0)
    mixed = dot_last(left, x_norm)
    query_t = mixed[: H * rows]
    key_t = mixed[H * rows : 2 * H * rows] / math.sqrt(DK)
    input_pre = mixed[2 * H * rows : 2 * H * rows + H] + column(bi_ref[...])
    forget_pre = mixed[2 * H * rows + H :] + column(bf_ref[...])
    log_forget = jnp.minimum(forget_pre, 0.0) - jnp.log1p(jnp.exp(-jnp.abs(forget_pre)))
    kept = log_forget + stab_ref[...]
    stab_new = jnp.maximum(kept, input_pre)
    input_gate = jnp.exp(input_pre - stab_new)
    forget_gate = jnp.exp(kept - stab_new)
    stab_out_ref[...] = stab_new
    fg_ref[...] = forget_gate
    ig_ref[...] = input_gate

    for h in range(H):
        part = slice(h * rows, (h + 1) * rows)
        key_h = key_t[part]
        query_h = query_t[part]
        f_h = jnp.broadcast_to(forget_gate[h : h + 1], (rows, batch))
        ik_h = input_gate[h : h + 1] * key_h
        norm_h = f_h * nrm_ref[part] + ik_h
        nrm_out_ref[part] = norm_h
        f_rows_ref[part] = f_h
        ik_rows_ref[part] = ik_h
        norm_query = jnp.sum(norm_h * query_h, axis=0, keepdims=True)
        key_query = jnp.sum(key_h * query_h, axis=0, keepdims=True)
        kinds = (*split_hi_lo(norm_query), *split_hi_lo(key_query))
        for k, kind in enumerate(kinds):
            tail_ref[h, 4 + k : 5 + k, :batch] = kind

    spread = batch * rows
    high, low = split_hi_lo(query_t.T)
    both = jnp.concatenate([high, low], axis=0).astype(BF16)
    spread = repeat_ref.shape[1] // H
    wide = dot(both, repeat_ref[...]).astype(BF16)
    share = pieces // H
    deep = 2 * rows
    for h in range(H):
        wide_h = wide[:, h * spread : (h + 1) * spread]
        left = jnp.concatenate([wide_h, wide_h], axis=0) * own_ref[...]
        right = [mem_ref[:, h, k * deep : (k + 1) * deep].reshape(spread, width) for k in range(2)]
        product = dot(left, jnp.concatenate(right, axis=1))
        for parity in range(2):
            at = parity * 2 * batch
            numer = (product[at : at + batch] + product[at + batch : at + 2 * batch]).astype(BF16)
            for k in range(2):
                out_ref[SLOT[h * share + 2 * k + parity], :batch] = numer[:, k * width : (k + 1) * width]

    value = value_gate[:, :width]
    top = lax.broadcasted_iota(jnp.int32, (8, width), 0) < 4
    for core in range(2):
        first = value[core * half : core * half + 8].astype(BF16)
        rest = value[core * half + 8 : (core + 1) * half]
        rest = jnp.concatenate([rest, rest], axis=0)
        tails = [jnp.where(top, rest, tail_ref[h]).astype(BF16) for h in range(H)]
        for j in range(core, pieces, 2):
            out_ref[SLOT[j], batch : batch + 8] = first
            out_ref[SLOT[j], batch + 8 :] = tails[j // share]

    head = lax.axis_index("head") * width // DV
    pick = lambda ref: column(ref[pl.ds(head, 1), :])
    gate = jax.nn.sigmoid(value_gate[:, width:])
    sum_scale_ref[...] = gate * pick(fg_ref)
    own_value_ref[...] = gate * (pick(ig_ref) * value.astype(BF16).astype(F32))
    floor_ref[...] = jnp.broadcast_to(jnp.exp(-pick(stab_out_ref)), floor_ref.shape)


def output_kernel(in_ref, sum_scale_ref, own_ref, floor_ref, wo_ref, out_ref):
    pieces, batch, width = out_ref.shape
    total = in_ref[0, :batch].astype(F32)
    tail = in_ref[0, batch + 8 :].astype(F32)
    for j in range(1, pieces):
        total = total + in_ref[j, :batch].astype(F32)
        tail = tail + in_ref[j, batch + 8 :].astype(F32)
    norm_query = column(tail[4:5, :batch] + tail[5:6, :batch])
    key_query = column(tail[6:7, :batch] + tail[7:8, :batch])
    numer = sum_scale_ref[...] * total + own_ref[...] * key_query
    hidden = (numer / jnp.maximum(jnp.abs(norm_query), floor_ref[...])).astype(BF16)
    for j in range(0, pieces, 2):
        pair = dot(hidden, wo_ref[:, j * width : (j + 2) * width]).astype(BF16)
        out_ref[SLOT[j]] = pair[:, :width]
        out_ref[SLOT[j + 1]] = pair[:, width:]


def memory_half(side, f_rows_ref, ik_rows_ref, half_ref, mem_ref, out_hbm, wide_ref, new_ref, sems):
    pieces, depth, width = half_ref.shape
    _, _, rows, _ = mem_ref.shape
    half = wide_ref.shape[1]
    share = pieces // H
    first = depth - 16
    lower = lax.axis_index("head") % 2 == side
    base = jnp.where(lower, 0, half)
    for j in range(pieces):
        cut = slice((j % share) * width, (j % share + 1) * width)
        wide_ref[j // share, :, cut] = half_ref[SLOT[j], first:].astype(F32)[:half]

    f_mine = jnp.where(lower, f_rows_ref[:, :half], f_rows_ref[:, half:])
    ik_mine = jnp.where(lower, ik_rows_ref[:, :half], ik_rows_ref[:, half:])
    step = half // CHUNKS
    copies = []
    for k in range(CHUNKS):
        for h in range(H):
            part = slice(h * rows, (h + 1) * rows)
            for i in range(k * step, (k + 1) * step):
                kept = f_mine[part, i : i + 1] * mem_ref[base + i, h].astype(F32)
                added = ik_mine[part, i : i + 1] * wide_ref[h, i : i + 1, :]
                new_ref[i, h] = (kept + added).astype(BF16)
        source = new_ref.at[k * step : (k + 1) * step]
        target = out_hbm.at[pl.ds(base + k * step, step)]
        copies.append(pltpu.make_async_copy(source, target, sems.at[k]))
        copies[-1].start()
    for copy in copies:
        copy.wait()


def memory_mine_kernel(
    f_rows_ref, ik_rows_ref, norm_ref, stab_ref, half_ref, mem_ref,
    out_hbm, norm_out_hbm, stab_out_hbm, wide_ref, new_ref, sems, small_sems,
):
    norm_copy = pltpu.make_async_copy(norm_ref, norm_out_hbm, small_sems.at[0])
    stab_copy = pltpu.make_async_copy(stab_ref, stab_out_hbm, small_sems.at[1])
    norm_copy.start()
    stab_copy.start()
    memory_half(0, f_rows_ref, ik_rows_ref, half_ref, mem_ref, out_hbm, wide_ref, new_ref, sems)
    norm_copy.wait()
    stab_copy.wait()


def memory_other_kernel(
    f_rows_ref, ik_rows_ref, half_ref, mem_ref, partial_hbm, out_hbm, wide_ref, new_ref, sems
):
    del partial_hbm
    memory_half(1, f_rows_ref, ik_rows_ref, half_ref, mem_ref, out_hbm, wide_ref, new_ref, sems)


def finish_kernel(in_ref, residual_ref, out_ref):
    total = residual_ref[...]
    acc = in_ref[0].astype(F32)
    for j in range(1, in_ref.shape[0]):
        acc = acc + in_ref[j].astype(F32)
    out_ref[...] = total + acc


def call(kernel, outs, n_in, scratch=(), flops=1_000_000, hbm_out=False, alias=False):
    vmem, hbm = (pl.BlockSpec(memory_space=space) for space in (pltpu.VMEM, pltpu.HBM))
    return pl.pallas_call(
        kernel,
        out_shape=[jax.ShapeDtypeStruct(*out) for out in outs],
        in_specs=[vmem] * n_in + [hbm] * alias,
        out_specs=[hbm if hbm_out else vmem] * len(outs),
        scratch_shapes=list(scratch),
        input_output_aliases={n_in: 0} if alias else {},
        compiler_params=pltpu.CompilerParams(vmem_limit_bytes=16 * 2**20),
        cost_estimate=pl.CostEstimate(flops=flops, bytes_accessed=2_000_000, transcendentals=0),
    )


def body(
    residual,
    norm_gain,
    w_query,
    w_key,
    w_value,
    w_gate,
    w_input,
    w_forget,
    b_input,
    b_forget,
    w_out,
    memory,
    normalizer,
    stabilizer,
):
    count = lax.axis_size("head")
    batch, width = residual.shape
    rows = w_query.shape[1]
    features = count * width
    (pieces,) = call(spread_kernel, [((count, batch, width), BF16)], 1, flops=SPREAD_FLOPS)(residual)
    gathered = exchange(pieces)

    piece = ((count, batch, width), BF16)
    sources = (
        norm_gain[None],
        w_input,
        w_forget,
        b_input[None],
        b_forget[None],
        normalizer.transpose(1, 2, 0).reshape(H * rows, batch),
        stabilizer.T,
        w_query.reshape(H * rows, features),
        w_key.reshape(H * rows, features),
        w_value,
        w_gate,
        memory.reshape(batch, H, rows, DV // width, width)
        .transpose(0, 1, 3, 2, 4)
        .reshape(batch, H, DV // width * rows, width),
        repeat_matrix(rows, batch),
        own_mask(rows, batch),
    )
    payload, norm_new, stab_new, f_rows, ik_rows, sum_scale, own, floor = call(
        project_kernel,
        [
            ((count, batch + batch // 2 + 4, width), BF16),
            ((H * rows, batch), F32),
            ((H, batch), F32),
            ((H * rows, batch), F32),
            ((H * rows, batch), F32),
            ((batch, width), F32),
            ((batch, width), F32),
            ((batch, width), F32),
        ],
        1 + len(sources),
        scratch=[
            pltpu.VMEM((batch, features), BF16),
            pltpu.VMEM((H, 8, width), F32),
            pltpu.VMEM((H, batch), F32),
            pltpu.VMEM((H, batch), F32),
        ],
        flops=100_000_000,
    )(gathered, *sources)
    arrived = exchange(payload)
    (branch,) = call(output_kernel, [piece], 5, flops=30_000_000)(
        arrived, sum_scale, own, floor, w_out
    )
    returned = exchange(branch)
    with jax.named_scope("swap"):
        other = lax.ppermute(arrived[:, batch:], "head", [(i, i ^ 1) for i in range(count)])
    half_scratch = [
        pltpu.VMEM((H, batch // 2, DV), F32),
        pltpu.VMEM((batch // 2, *memory.shape[1:]), BF16),
        pltpu.SemaphoreType.DMA((CHUNKS,)),
    ]
    mem_half, norm_out, stab_out = call(
        memory_mine_kernel,
        [(memory.shape, BF16), ((H * rows, batch), F32), ((H, batch), F32)],
        6,
        scratch=[*half_scratch, pltpu.SemaphoreType.DMA((2,))],
        flops=50_000_000,
        hbm_out=True,
    )(f_rows, ik_rows, norm_new, stab_new, arrived, memory)
    (mem_new,) = call(
        memory_other_kernel,
        [(memory.shape, BF16)],
        4,
        scratch=half_scratch,
        flops=50_000_000,
        hbm_out=True,
        alias=True,
    )(f_rows, ik_rows, other, memory, mem_half)
    (res_out,) = call(finish_kernel, [((batch, width), F32)], 2)(returned, residual)
    norm_out = norm_out.reshape(H, rows, batch).transpose(2, 0, 1)
    return res_out, mem_new, norm_out, stab_out.T


def solution(mesh):
    in_specs = (
        P("dp", "head"),
        P(),
        P(None, "head", None),
        P(None, "head", None),
        P(None, "head"),
        P(None, "head"),
        P(),
        P(),
        P(),
        P(),
        P("head", None),
        P("dp", None, "head", None),
        P("dp", None, "head"),
        P("dp", None),
    )
    out_specs = (P("dp", "head"), P("dp", None, "head", None), P("dp", None, "head"), P("dp", None))
    return jax.shard_map(body, mesh=mesh, in_specs=in_specs, out_specs=out_specs, check_vma=False)
```
